32 devices in a mesh: gx: 8 (over y, x, core), gy: 4 (over z).
Axes of the slice: x: 2, y: 2, z: 4, core: 2. Of those that a mesh axis runs over, the one named last changes fastest.
Arguments:
- spectrum: float32 [192, 160, 1080], P('gx', 'gy'), may hold values from 0.05 to 1
- adjoint_in: float32 [192, 160, 1080], P('gx', 'gy'), may hold values from 0 to 2
- current_x: float32 [192, 160], P('gx', 'gy'), may hold values from -0.08 to 0.08
- current_y: float32 [192, 160], P('gx', 'gy'), may hold values from -0.08 to 0.08
- wind_x: float32 [192, 160], P('gx', 'gy'), may hold values from -4 to 4
- wind_y: float32 [192, 160], P('gx', 'gy'), may hold values from -4 to 4
- land_mask: int32 [192, 160], P('gx', 'gy'), may hold values from 0 to 1, as said below
- ice_mask: int32 [192, 160], P('gx', 'gy'), may hold values from 0 to 1, as said below
- group_speed: float32 [30], replicated, may hold values from 0.1 to 0.4
- growth_rate: float32 [30], replicated, may hold values from 0.1 to 1
- dissipation: float32 [30], replicated, may hold values from 0.3 to 3
Outputs:
- adjoint_spectrum: float32 [192, 160, 1080], P('gx', 'gy')
The draws below stay inside these ranges and needn't reach their ends.
Inputs may be any that keep to these rules, and one draw needn't show every extreme that they name: `land_mask`: 1 marks land, 0 sea. `ice_mask`: 1 marks sea ice, 0 open water.
All inputs are finite; a program needn't handle non-finite values.
Results may differ from the reference program's by a relative error of at most 0.0001.
Values sent between devices are 32-bit elements; how exact they have to be, the bound alone decides.
A program may use at most 128 MiB of HBM per device.

```python
import math
import jax
import jax.numpy as jnp
from jax import lax

DIRS = 36
FREQS = 30
BINS = 1080
CX = 24
CY = 40
NX = 192
NY = 160


def draw_land_mask(key, part):
    islands = max(2, NX * NY // (8 * CX * CY))
    centre_x = jax.random.randint(jax.random.fold_in(key, 1), (islands,), 0, NX)
    centre_y = jax.random.randint(jax.random.fold_in(key, 2), (islands,), 0, NY)
    radius = jax.random.randint(jax.random.fold_in(key, 3), (islands,), max(1, min(CX, CY) // 2), max(CX, CY) + 1)
    row_index = jnp.arange(NX, dtype=jnp.int32)
    col_index = jnp.arange(NY, dtype=jnp.int32)
    gap_x = jnp.abs(row_index[None, :] - centre_x[:, None])
    gap_x = jnp.minimum(gap_x, NX - gap_x)
    gap_y = jnp.abs(col_index[None, :] - centre_y[:, None])
    inside = gap_x[:, :, None] * gap_x[:, :, None] + gap_y[:, None, :] * gap_y[:, None, :] < (radius * radius)[:, None, None]
    return jnp.any(inside, axis=0).astype(jnp.int32)


def draw_ice_mask(key, part):
    ice_reach = max(2, NY // 8)
    south_edge = jax.random.randint(jax.random.fold_in(key, 11), (NX, 1), 0, ice_reach)
    north_edge = jax.random.randint(jax.random.fold_in(key, 12), (NX, 1), 0, ice_reach)
    col_index = jnp.arange(NY, dtype=jnp.int32)[None, :]
    frozen = (col_index < south_edge) | (col_index >= NY - north_edge)
    return frozen.astype(jnp.int32)


def shard_levels(own_key, extent, split, smallest, largest):
    gain = 1.0
    for axis_at, blocks in split:
        heights = jax.random.uniform(jax.random.fold_in(jax.random.fold_in(own_key, 6), axis_at), (blocks,), jnp.float32, smallest / len(split), largest / len(split))
        gain = gain * jnp.repeat(jnp.exp(heights), extent[axis_at] // blocks).reshape((-1,) + (1,) * (len(extent) - 1 - axis_at))
    return gain


def bell_draw(own_key, shape, scale, most, split=(), held_as=jnp.bfloat16):
    loudness = shard_levels(own_key, shape, split, -0.22, 0.18) if split else 1.0
    entries = jax.random.normal(own_key, shape, jnp.float32) * scale * loudness
    return jnp.minimum(jnp.maximum(entries, -most), most).astype(held_as)


def setup_inputs(seed: int = 0) -> dict:
    key_of = jax.random.split(jax.random.key(seed), 12)
    return {
        "spectrum": jnp.clip(jnp.exp(math.log(1.0) - 2.9957323 * jax.random.uniform(key_of[0], (NX, NY, BINS), jnp.float32) ** shard_levels(key_of[0], (NX, NY, BINS), ((0, 8), (1, 4)), -0.2, 0.2)), 0.05, 1.0),
        "adjoint_in": jnp.clip(2.0 * jax.random.uniform(key_of[1], (NX, NY, BINS), jnp.float32) ** shard_levels(key_of[1], (NX, NY, BINS), ((0, 8), (1, 4)), -0.2, 0.2), 0.0, 2.0),
        "current_x": jnp.clip(jax.random.uniform(key_of[2], (NX, NY), jnp.float32, -0.08, 0.08) * shard_levels(key_of[2], (NX, NY), ((0, 8), (1, 4)), -0.4, 0.0), -0.08, 0.08),
        "current_y": jnp.clip(jax.random.uniform(key_of[3], (NX, NY), jnp.float32, -0.08, 0.08) * shard_levels(key_of[3], (NX, NY), ((0, 8), (1, 4)), -0.4, 0.0), -0.08, 0.08),
        "wind_x": bell_draw(key_of[4], (NX, NY), 1.0, 4.0, ((0, 8), (1, 4)), jnp.float32),
        "wind_y": bell_draw(key_of[5], (NX, NY), 1.0, 4.0, ((0, 8), (1, 4)), jnp.float32),
        "land_mask": draw_land_mask(jax.random.fold_in(key_of[11], 71), 0),
        "ice_mask": draw_ice_mask(jax.random.fold_in(key_of[11], 71), 0),
        "group_speed": jnp.clip(jnp.exp(jax.random.uniform(key_of[8], (FREQS,), jnp.float32, math.log(0.1), math.log(0.4))), 0.1, 0.4),
        "growth_rate": jnp.clip(jnp.exp(jax.random.uniform(key_of[9], (FREQS,), jnp.float32, math.log(0.1), math.log(1.0))), 0.1, 1.0),
        "dissipation": jnp.clip(jnp.exp(jax.random.uniform(key_of[10], (FREQS,), jnp.float32, math.log(0.3), math.log(3.0))), 0.3, 3.0),
    }


def shift_north(values):
    return jnp.concatenate([values[:, 1:], jnp.zeros_like(values[:, :1])], axis=1)


def shift_south(values):
    return jnp.concatenate([jnp.zeros_like(values[:, :1]), values[:, :-1]], axis=1)


def reference(spectrum, adjoint_in, current_x, current_y, wind_x, wind_y, land_mask, ice_mask, group_speed, growth_rate, dissipation):
    sea_mask = (1 - land_mask).astype(jnp.float32)
    ice_free = (1 - ice_mask).astype(jnp.float32)
    angles = (2.0 * math.pi / DIRS) * (jnp.arange(DIRS, dtype=jnp.float32) + 0.5)
    open_lon = sea_mask * jnp.roll(sea_mask, -1, axis=0)
    drift_lon = 0.5 * (current_x + jnp.roll(current_x, -1, axis=0))
    open_lat = sea_mask * shift_north(sea_mask)
    drift_lat = 0.5 * (current_y + shift_north(current_y))

    def forward_block(direction):
        offset = (direction * FREQS).astype(jnp.int32)
        block_field = lax.dynamic_slice_in_dim(spectrum, offset, FREQS, 2)
        cosine = jnp.cos(angles[direction])
        sine_val = jnp.sin(angles[direction])
        lon_courant = open_lon[..., None] * (group_speed * cosine + drift_lon[..., None])
        lat_courant = open_lat[..., None] * (group_speed * sine_val + drift_lat[..., None])
        lon_plus = jnp.maximum(lon_courant, 0.0)
        lon_minus = jnp.minimum(lon_courant, 0.0)
        lat_plus = jnp.maximum(lat_courant, 0.0)
        lat_minus = jnp.minimum(lat_courant, 0.0)
        lon_flux = lon_plus * block_field + lon_minus * jnp.roll(block_field, -1, axis=0)
        lat_flux = lat_plus * block_field + lat_minus * shift_north(block_field)
        advected = block_field - (lon_flux - jnp.roll(lon_flux, 1, axis=0)) - (lat_flux - shift_south(lat_flux))
        return advected, lon_plus, lon_minus, lat_plus, lat_minus, offset, cosine, sine_val

    def add_energy(direction, running):
        advected = forward_block(direction)[0]
        return running + jnp.sum(advected, axis=2)

    energy = lax.fori_loop(0, DIRS, add_energy, jnp.zeros((NX, NY), jnp.float32)) / BINS

    def weigh_block(direction):
        advected, lon_plus, lon_minus, lat_plus, lat_minus, offset, cosine, sine_val = forward_block(direction)
        incoming = lax.dynamic_slice_in_dim(adjoint_in, offset, FREQS, 2)
        project = wind_x[..., None] * cosine + wind_y[..., None] * sine_val
        gained = 1.0 + growth_rate * jnp.maximum(project, 0.0) * ice_free[..., None]
        damped = 1.0 + dissipation * energy[..., None] * advected
        weighted = incoming * gained / (damped * damped)
        return advected, weighted, lon_plus, lon_minus, lat_plus, lat_minus, offset

    def add_coupling(direction, running):
        parts = weigh_block(direction)
        advected, weighted = parts[0], parts[1]
        return running + jnp.sum(weighted * dissipation * advected * advected, axis=2)

    coupling = lax.fori_loop(0, DIRS, add_coupling, jnp.zeros((NX, NY), jnp.float32))

    def adjoint_block(direction, output):
        advected, weighted, lon_plus, lon_minus, lat_plus, lat_minus, offset = weigh_block(direction)
        sensitivity = sea_mask[..., None] * (weighted - coupling[..., None] / BINS)
        lon_step = jnp.roll(sensitivity, -1, axis=0) - sensitivity
        lat_step = shift_north(sensitivity) - sensitivity
        result = sensitivity + lon_plus * lon_step + jnp.roll(lon_minus * lon_step, 1, axis=0)
        result = result + lat_plus * lat_step + shift_south(lat_minus * lat_step)
        return lax.dynamic_update_slice_in_dim(output, result, offset, 2)

    return lax.fori_loop(0, DIRS, adjoint_block, jnp.zeros((NX, NY, BINS), jnp.float32))
```

```python
import functools
import math
from types import SimpleNamespace

import jax
import jax.numpy as jnp
import numpy as np
from jax import lax
from jax.experimental import pallas as pl
from jax.experimental.pallas import tpu as pltpu
from jax.sharding import PartitionSpec as P

DIRS = 36
LANES = 128
TILE = 8
CERTAIN = 0.81
HBM = pl.BlockSpec(memory_space=pltpu.HBM)
VMEM = pl.BlockSpec(memory_space=pltpu.VMEM)
MESH = pl.DeviceIdType.MESH


def lane_chunks(bins):
    return [(c, s, min(LANES, bins - s)) for c, s in enumerate(range(0, bins, LANES))]


def slot_plan(need):
    parts = []
    for c, s, w in lane_chunks(len(need)):
        lane = 0
        while lane < w:
            if not need[s + lane]:
                lane += 1
                continue
            first = lane
            while lane < w and need[s + lane]:
                lane += 1
            parts.append((c, first, lane, w))
    parts.sort(key=lambda p: (p[3] == LANES, p[1] - p[2]))
    slots, used = [], []
    for c, first, last, w in parts:
        size = last - first
        for n, busy in enumerate(used):
            if not busy[first:last].any():
                shift = 0
            elif w == LANES:
                starts = [k for k in range(LANES - size + 1) if not busy[k : k + size].any()]
                if not starts:
                    continue
                shift = starts[0] - first
            else:
                continue
            busy[first + shift : last + shift] = True
            slots[n].append((c, first, last, shift % LANES))
            break
        else:
            busy = np.zeros(LANES, bool)
            busy[first:last] = True
            used.append(busy)
            slots.append([(c, first, last, 0)])
    return slots


def repeat(value, count):
    return value if count == 1 else jnp.concatenate([value] * count, axis=0)


def between(first, last):
    lane = lax.broadcasted_iota(jnp.int32, (TILE, LANES), 1)
    return jnp.logical_and(lane >= first, lane < last)


def pack(plan, chunks, load, out):
    for n, parts in enumerate(plan):
        value, late = None, None
        for c, first, last, shift in parts:
            w = chunks[c][2]
            if w < LANES:
                late = (c, w)
                continue
            part = load(c)
            if shift:
                part = pltpu.roll(part, shift, axis=1)
            begin = (first + shift) % LANES
            value = part if value is None else jnp.where(between(begin, begin + last - first), part, value)
        if value is not None:
            out[n] = value
        if late is not None:
            out[n, :, 0 : late[1]] = load(late[0])


def unpack(plan, chunk, slots):
    c, _, w = chunk
    value = jnp.zeros((TILE, w), jnp.float32)
    for n, parts in enumerate(plan):
        for chunk_of, first, last, shift in parts:
            if chunk_of != c:
                continue
            if w < LANES:
                part = slots[n, :, 0:w]
                if last - first < w:
                    part = jnp.where(between(first, last)[:, 0:w], part, 0.0)
                value = part
                continue
            part = slots[n]
            if shift:
                part = pltpu.roll(part, LANES - shift, axis=1)
            value = part if last - first == LANES else jnp.where(between(first, last), part, value)
    return value


def split3(value):
    high = value.astype(jnp.bfloat16).astype(jnp.float32)
    rest = value - high
    mid = rest.astype(jnp.bfloat16).astype(jnp.float32)
    return [high, mid, rest - mid]


def kernel(
    nx, ny, plan_pos, plan_neg, lat_groups,
    spectrum, adjoint, cx_h, cy_h, wx_h, wy_h, land_h, ice_h, speed_h, growth_h, diss_h, consts_h,
    done,
    both, lat, rim, tt, cxs, fxs, cys, tab, opx, odx, opy, ody, wxs, wys, seas,
    send_s, recv_s, send_t, recv_t, mine_f, mine_i, near_f, near_i, face_f, face_i, coeffs, consts, params, ext, bufs, load_sem, send_sem, recv_sem,
):
    gx, gy = lax.axis_index("gx"), lax.axis_index("gy")
    rows, cells, bins = adjoint.shape
    east, west = lax.rem(gx + 1, nx), lax.rem(gx + nx - 1, nx)
    has_north, has_south = gy < ny - 1, gy > 0
    chunks = lane_chunks(bins)
    tiles = cells // TILE
    f32 = jnp.float32
    sp, adj = both.at[0], both.at[1]

    cx, cy, wx, wy = (mine_f.at[m] for m in range(4))
    land, ice = (mine_i.at[m] for m in range(2))
    speed, growth, diss = (coeffs.at[m] for m in range(3))
    pairs = (rows - 2) // 2
    bounds = [1, 4, 10, 16, rows - 1]
    local = lambda src, dst, n: pltpu.make_async_copy(src, dst, load_sem.at[n])
    ends = [local(spectrum.at[r], sp.at[r], 0) for r in (0, rows - 1)]
    small = [
        local(src, dst, n)
        for src, dst, n in (
            (cx_h, cx, 1), (cy_h, cy, 1), (wx_h, wx, 1), (wy_h, wy, 1), (land_h, land, 2), (ice_h, ice, 2),
            (speed_h, speed, 3), (growth_h, growth, 3), (diss_h, diss, 3), (consts_h, consts, 4),
        )
    ]
    rims = [
        local(spectrum.at[:, pl.ds(0, 1), :], rim.at[0], 5),
        local(spectrum.at[:, pl.ds(cells - 1, 1), :], rim.at[1], 5),
    ]
    groups = []
    for n, (a, b) in enumerate(zip(bounds[:-1], bounds[1:])):
        groups.append(
            [local(src.at[pl.ds(a, b - a)], dst.at[pl.ds(a, b - a)], 6 + n) for src, dst in ((spectrum, sp), (adjoint, adj))]
        )
    last_adj = [local(adjoint.at[r], adj.at[r], 6 + len(groups)) for r in (0, rows - 1)]
    for copy in ends + small + rims:
        copy.start()

    barrier = pltpu.get_barrier_semaphore()
    for where in (east, west):
        pl.semaphore_signal(barrier, inc=1, device_id={"gx": where}, device_id_type=MESH)

    @pl.when(has_north)
    def _():
        pl.semaphore_signal(barrier, inc=1, device_id={"gy": gy + 1}, device_id_type=MESH)

    @pl.when(has_south)
    def _():
        pl.semaphore_signal(barrier, inc=1, device_id={"gy": gy - 1}, device_id_type=MESH)

    for group in groups:
        for copy in group:
            copy.start()
    for copy in last_adj:
        copy.start()

    def far(src, dst, out, n, axis, where):
        return pltpu.make_async_remote_copy(
            src_ref=src, dst_ref=dst, send_sem=send_sem.at[out], recv_sem=recv_sem.at[n],
            device_id={axis: where}, device_id_type=MESH,
        )

    def settle(ref, sem):
        pltpu.make_async_copy(ref, ref, sem).wait()

    order = list(range(1, tiles - 1)) + [0, tiles - 1]
    ahead = []
    for m, (src, dst) in enumerate(((cx, face_f), (land, face_i))):
        ahead.append(far(src.at[pl.ds(rows - TILE, TILE)], dst.at[0], m, m, "gx", east))
        ahead.append(far(src.at[pl.ds(0, TILE)], dst.at[1], m, m, "gx", west))
    lon_s, lon_t = (
        [[far(src.at[p, d], dst.at[p, d], 2 + m, 2 + m * tiles + p, "gx", (east, west)[d]) for d in range(2)] for p in range(tiles)]
        for m, (src, dst) in enumerate(((send_s, recv_s), (send_t, recv_t)))
    )
    split = lat_groups[1][0]
    halves = ((0, split), (split, rows))
    spans = [[g] for g in lat_groups] + [[(0, 1), (rows - 1, rows)]]
    lat_all = []
    for d, (where, there, back_there) in enumerate(((gy + 1, has_north, has_south), (gy - 1, has_south, has_north))):
        sem = 2 + 2 * tiles + 7 * d
        away = lambda src, dst, out, n, where=where, d=d, sem=sem: far(src, dst, 4 + 4 * d + out, sem + n, "gy", where)
        own, halo = ((7 + cells, 7), (8, 8 + cells))[d]
        small_lat = [away(cy, near_f.at[d], 0, 0), away(land, near_i.at[d], 1, 1)]
        first = [away(rim.at[1 - d, pl.ds(a, b - a)], lat.at[d, pl.ds(a, b - a)], 2, 2 + n) for n, (a, b) in enumerate(halves)]
        second = [
            [away(tt.at[pl.ds(a, b - a), :, pl.ds(own, 1)], tt.at[pl.ds(a, b - a), :, pl.ds(halo, 1)], 3, 4 + n) for a, b in span]
            for n, span in enumerate(spans)
        ]
        lat_all.append(SimpleNamespace(
            there=there, back_there=back_there, small=small_lat, first=first, second=second, sem=sem, out=4 + 4 * d, own=own, halo=halo,
        ))

    def lat_start(pick):
        for side in lat_all:
            @pl.when(side.there)
            def _(side=side):
                for copy in pick(side):
                    copy.start()

    def lat_arrive(pick):
        for side in lat_all:
            @pl.when(side.back_there)
            def _(side=side):
                pick(side)

    def first_arrives(n):
        lat_arrive(lambda side: side.first[n].wait_recv())

    def second_arrives(n):
        count = sum(b - a for a, b in spans[n])
        lat_arrive(lambda side: settle(tt.at[pl.ds(0, count), :, pl.ds(side.halo, 1)], recv_sem.at[side.sem + 4 + n]))

    settle(sp.at[pl.ds(0, 2)], load_sem.at[0])
    for p in range(tiles):
        for d, (row, plan) in enumerate(((rows - 1, plan_pos), (0, plan_neg))):
            load = lambda c, row=row, p=p: sp[row, TILE * p : TILE * p + TILE, chunks[c][1] : chunks[c][1] + chunks[c][2]]
            pack(plan, chunks, load, send_s.at[p, d])
    for n, ref in enumerate((mine_f, mine_i, coeffs, consts, rim)):
        settle(ref, load_sem.at[1 + n])

    freqs = coeffs.shape[2]
    params[...] = jnp.zeros(params.shape, f32)
    for m, ref in enumerate((speed, growth, diss)):
        params[TILE * m : TILE * m + TILE, 0:freqs] = jnp.broadcast_to(ref[...], (TILE, freqs))
    pl.semaphore_wait(barrier, 2 + has_north.astype(jnp.int32) + has_south.astype(jnp.int32))
    for copy in ahead:
        copy.start()
    lat_start(lambda side: side.small)
    for p in order:
        for copy in lon_s[p]:
            copy.start()
    lat_start(lambda side: side.first)

    many = params.shape[1]
    hot = consts[0:many].astype(jnp.bfloat16)
    by_bin = sum(
        jnp.dot(part.astype(jnp.bfloat16), hot, preferred_element_type=f32) for part in split3(params[...])
    )
    cosine, sine = consts[many : many + TILE], consts[many + TILE : many + 2 * TILE]
    for c, s, w in chunks:
        cs = slice(s, s + w)
        tab[0, c, :, 0:w] = by_bin[0:TILE, cs] * cosine[:, cs]
        tab[1, c, :, 0:w] = by_bin[0:TILE, cs] * sine[:, cs]
        tab[2, c, :, 0:w] = by_bin[TILE : 2 * TILE, cs] * cosine[:, cs]
        tab[3, c, :, 0:w] = by_bin[TILE : 2 * TILE, cs] * sine[:, cs]
        tab[4, c, :, 0:w] = by_bin[2 * TILE : 3 * TILE, cs]

    sub = lax.broadcasted_iota(jnp.int32, (LANES, 2 * LANES), 0)
    half = (lax.broadcasted_iota(jnp.int32, (LANES, 2 * LANES), 1) >= LANES).astype(jnp.int32)
    row_of = jnp.where(sub < rows, sub, jnp.where(sub < 2 * rows, sub - rows, jnp.where(sub < 3 * rows, sub - 2 * rows, -2)))
    row_of = row_of - half

    def turned(field):
        stack = split3(field)
        stack.append(jnp.zeros((LANES - 3 * rows, LANES), f32))
        return jnp.concatenate(stack, axis=0).T

    def spread(lhs, count, put):
        lhs = lhs.astype(jnp.bfloat16)
        for n in range(count // 2):
            pick = jnp.where(row_of == 2 * n, 1.0, 0.0).astype(jnp.bfloat16)
            out = jnp.dot(lhs, pick, preferred_element_type=f32)
            put(2 * n, out[:, 0:LANES])
            put(2 * n + 1, out[:, LANES:])

    sea_of = lambda mask: (1 - mask).astype(f32)
    ext[...] = jnp.zeros(ext.shape, f32)
    ice_free = sea_of(ice[...])
    ext[0, 1 : rows + 1, 0:cells] = cx[...]
    ext[1, 1 : rows + 1, 0:cells] = sea_of(land[...])
    ext[2, 0:rows, 0:cells] = cy[...]
    ext[3, 0:rows, 0:cells] = sea_of(land[...])
    ext[8, 0:rows, 0:cells] = wx[...] * ice_free
    ext[9, 0:rows, 0:cells] = wy[...] * ice_free
    lane = lax.broadcasted_iota(jnp.int32, (rows, LANES), 1)
    sea, drift = ext[3, 0:rows], ext[2, 0:rows]
    opened_x = ext[1, 0:rows] * ext[1, 1 : rows + 1]
    ahead_of = lambda value: pltpu.roll(value, LANES - 1, axis=1)
    opened_y = sea * ahead_of(sea)
    fields = [
        opened_x, opened_x * (0.5 * (ext[0, 0:rows] + ext[0, 1 : rows + 1])),
        opened_y, opened_y * (0.5 * (drift + ahead_of(drift))),
        ext[8, 0:rows], ext[9, 0:rows], sea,
    ]
    homes = (opx, odx, opy, ody, wxs, wys, seas)

    def put_all(i, block):
        for k, home in enumerate(homes):
            home[i, 0:cells] = block[k * cells : (k + 1) * cells]

    spread(jnp.concatenate([turned(f)[0:cells] for f in fields], axis=0), rows, put_all)

    @pl.when(jnp.logical_not(has_south))
    def _():
        lat[0] = jnp.zeros(lat.shape[1:], f32)

        def clear(r, carry):
            for c, _, _ in chunks:
                tt[r, c, 7:8] = jnp.zeros((1, LANES), f32)
            return carry

        lax.fori_loop(0, rows, clear, 0)

    @pl.when(jnp.logical_not(has_north))
    def _():
        lat[1] = jnp.zeros(lat.shape[1:], f32)

        def clear(r, carry):
            for c, _, _ in chunks:
                tt[r, c, 8 + cells : 9 + cells] = jnp.zeros((1, LANES), f32)
            return carry

        lax.fori_loop(0, rows, clear, 0)

    def lat_part(buf, r, chunk, lo, hi, own):
        c, s, w = chunk
        count = (hi - lo) // TILE
        sine_row = tab[1, c, :, 0:w]
        buf.near[c, lo:hi, 0:w] = own
        buf.near[c, hi : hi + 1, 0:w] = sp[r, hi : hi + 1, s : s + w] if hi < cells else lat[1, r, :, s : s + w]
        upper = buf.near[c, lo + 1 : hi + 1, 0:w]
        courant = opy[r, lo:hi, 0:w] * repeat(sine_row, count) + ody[r, lo:hi, 0:w]
        cys[r, c, 8 + lo : 8 + hi, 0:w] = courant
        fy = courant * jnp.where(courant > 0, own, upper)
        buf.flux[c, 8 + lo : 8 + hi, 0:w] = fy
        at = lo - 1 if lo else cells
        low = opy[r, at : at + 1, 0:w] * sine_row[0:1] + ody[r, at : at + 1, 0:w]
        below = sp[r, lo - 1 : lo, s : s + w] if lo else lat[0, r, :, s : s + w]
        cys[r, c, 7 + lo : 8 + lo, 0:w] = low
        buf.flux[c, 7 + lo : 8 + lo, 0:w] = low * jnp.where(low > 0, below, own[0:1])
        return fy - buf.flux[c, 7 + lo : 7 + hi, 0:w]

    def lon_speed(f, chunk, lo, hi):
        c, _, w = chunk
        speed = opx[f, lo:hi, 0:w] * repeat(tab[0, c, :, 0:w], (hi - lo) // TILE) + odx[f, lo:hi, 0:w]
        cxs[f, c, lo:hi, 0:w] = speed
        return speed

    def upwind(speed, here, there):
        return speed * jnp.where(speed > 0, here, there)

    def gather(totals, rest):
        value = jnp.sum(totals, axis=1, keepdims=True)
        return value if rest is None else value + rest

    def source(buf, r, segments, sums):
        for n, (lo, hi) in enumerate(segments):
            count = (hi - lo) // TILE
            energy = jnp.broadcast_to(gather(*sums[n]) * (1.0 / bins), (hi - lo, LANES))
            total, rest = jnp.zeros((hi - lo, LANES), f32), None
            for c, s, w in chunks:
                advected = buf.moved[c, lo:hi, 0:w]
                blow = wxs[r, lo:hi, 0:w] * repeat(tab[2, c, :, 0:w], count) + wys[r, lo:hi, 0:w] * repeat(tab[3, c, :, 0:w], count)
                gain = 1.0 + jnp.maximum(blow, 0.0)
                scaled = repeat(tab[4, c, :, 0:w], count) * advected
                damp = 1.0 + energy[:, 0:w] * scaled
                weighted = adj[r, lo:hi, s : s + w] * gain / (damp * damp)
                buf.weight[c, lo:hi, 0:w] = weighted
                term = weighted * scaled * advected
                if w == LANES:
                    total = total + term
                else:
                    rest = jnp.sum(term, axis=1, keepdims=True)
            sums[n] = (total, rest)
        yield
        for n, (lo, hi) in enumerate(segments):
            coupling = jnp.broadcast_to(gather(*sums[n]) * (1.0 / bins), (hi - lo, LANES))
            for c, s, w in chunks:
                tt[r, c, 8 + lo : 8 + hi, 0:w] = seas[r, lo:hi, 0:w] * (buf.weight[c, lo:hi, 0:w] - coupling[:, 0:w])
        yield

    slots = [SimpleNamespace(near=bufs.at[4 * q], flux=bufs.at[4 * q + 1], moved=bufs.at[4 * q + 2], weight=bufs.at[4 * q + 3]) for q in range(2)]

    def run(jobs):
        stages = [source(*job) for job in jobs]
        for _ in range(2):
            for stage in stages:
                next(stage)

    def store_moved(buf, chunk, lo, hi, moved, total, rest):
        c, _, w = chunk
        buf.moved[c, lo:hi, 0:w] = moved
        if w == LANES:
            return total + moved, rest
        return total, jnp.sum(moved, axis=1, keepdims=True)

    def row_pair(r, segments):
        sums = [[(jnp.zeros((hi - lo, LANES), f32), None) for lo, hi in segments] for _ in range(2)]
        for chunk in chunks:
            c, s, w = chunk
            for n, (lo, hi) in enumerate(segments):
                own = [sp[r + q, lo:hi, s : s + w] for q in range(3)]
                flux_west = fxs[0, c, lo:hi, 0:w]
                for q in range(2):
                    flux = upwind(lon_speed(r + q + 1, chunk, lo, hi), own[q], own[q + 1])
                    if q:
                        fxs[0, c, lo:hi, 0:w] = flux
                    moved = own[q] - (flux - flux_west) - lat_part(slots[q], r + q, chunk, lo, hi, own[q])
                    flux_west = flux
                    sums[q][n] = store_moved(slots[q], chunk, lo, hi, moved, *sums[q][n])
        run([(slots[q], r + q, segments, sums[q]) for q in range(2)])

    def edge(p):
        lo, hi = TILE * p, TILE * p + TILE
        sums = [[(jnp.zeros((TILE, LANES), f32), None)] for _ in range(2)]
        for chunk in chunks:
            c, s, w = chunk
            for q, r in enumerate((0, rows - 1)):
                own = sp[r, lo:hi, s : s + w]
                if q == 0:
                    flux_west = upwind(lon_speed(0, chunk, lo, hi), unpack(plan_pos, chunk, recv_s.at[p, 0]), own)
                    flux = fxs[1, c, lo:hi, 0:w]
                else:
                    flux_west = fxs[0, c, lo:hi, 0:w]
                    flux = upwind(lon_speed(rows, chunk, lo, hi), own, unpack(plan_neg, chunk, recv_s.at[p, 1]))
                moved = own - (flux - flux_west) - lat_part(slots[q], r, chunk, lo, hi, own)
                sums[q][0] = store_moved(slots[q], chunk, lo, hi, moved, *sums[q][0])
        run([(slots[q], r, [(lo, hi)], sums[q]) for q, r in enumerate((0, rows - 1))])
        for d, (row, plan) in enumerate(((rows - 1, plan_neg), (0, plan_pos))):
            pack(plan, chunks, lambda c, row=row: tt[row, c, 8 + lo : 8 + hi, 0 : chunks[c][2]], send_t.at[p, d])
        for copy in lon_t[p]:
            copy.start()

    def wait_group(n):
        settle(both.at[:, pl.ds(bounds[n], bounds[n + 1] - bounds[n])], load_sem.at[6 + n])

    wait_group(0)
    for chunk in chunks:
        c, s, w = chunk
        for lo in range(0, cells, TILE):
            flux = upwind(lon_speed(1, chunk, lo, lo + TILE), sp[0, lo : lo + TILE, s : s + w], sp[1, lo : lo + TILE, s : s + w])
            for m in range(2):
                fxs[m, c, lo : lo + TILE, 0:w] = flux

    inner = [(TILE, cells - TILE)]
    outer = [(0, TILE), (cells - TILE, cells)]
    firsts = [next(k for k in range(pairs + 1) if 3 + 2 * k >= b) for b in bounds[1:-1]]

    def inner_pair(k, carry):
        for n, first in enumerate(firsts):
            @pl.when(k == first)
            def _(n=n):
                wait_group(n + 1)

        row_pair(1 + 2 * k, inner)
        return carry

    def outer_pair(k, carry):
        row_pair(1 + 2 * k, outer)
        return carry

    lax.fori_loop(0, pairs, inner_pair, 0)
    for n in range(len(firsts)):
        if firsts[n] >= pairs:
            wait_group(n + 1)

    for m, ref in enumerate((face_f, face_i)):
        settle(ref, recv_sem.at[m])
    lat_arrive(lambda side: [copy.wait_recv() for copy in side.small])
    ext[0, 0:1, 0:cells] = face_f[0, TILE - 1 : TILE]
    ext[0, rows + 1 : rows + 2, 0:cells] = face_f[1, 0:1]
    ext[1, 0:1, 0:cells] = sea_of(face_i[0, TILE - 1 : TILE])
    ext[1, rows + 1 : rows + 2, 0:cells] = sea_of(face_i[1, 0:1])
    ext[4, 0:rows, 0:cells] = near_f[0]
    ext[5, 0:rows, 0:cells] = sea_of(near_i[0])
    ext[6, 0:rows, 0:cells] = near_f[1]
    ext[7, 0:rows, 0:cells] = sea_of(near_i[1])
    for n, f in enumerate((0, rows)):
        opened = ext[1, f : f + 1] * ext[1, f + 1 : f + 2]
        ext[10, n : n + 1] = opened
        ext[10, n + 2 : n + 3] = opened * (0.5 * (ext[0, f : f + 1] + ext[0, f + 1 : f + 2]))

    def put_lon(i, block):
        (opx, odx)[i // 2][(0, rows)[i % 2], 0:cells] = block

    spread(turned(ext[10, 0:rows])[0:cells], 4, put_lon)

    def with_ends(own, south, north):
        mine = jnp.where(lane == cells, pltpu.roll(own, cells, axis=1), own)
        other = jnp.where(lane == cells - 1, pltpu.roll(north, cells - 1, axis=1), ahead_of(own))
        return mine, jnp.where(lane == cells, pltpu.roll(south, 1, axis=1), other)

    sea_a, sea_b = with_ends(ext[3, 0:rows], ext[5, 0:rows], ext[7, 0:rows])
    cy_a, cy_b = with_ends(ext[2, 0:rows], ext[4, 0:rows], ext[6, 0:rows])
    closed = jnp.logical_or(
        jnp.logical_and(lane == cells, jnp.logical_not(has_south)),
        jnp.logical_and(lane == cells - 1, jnp.logical_not(has_north)),
    )
    opened = jnp.where(closed, 0.0, sea_a * sea_b)
    drift = jnp.where(closed, 0.0, opened * (0.5 * (cy_a + cy_b)))
    wide = slice(cells - TILE, cells + TILE)

    def put_lat(i, block):
        opy[i, wide] = block[0 : 2 * TILE]
        ody[i, wide] = block[2 * TILE : 4 * TILE]

    spread(jnp.concatenate([turned(opened)[wide], turned(drift)[wide]], axis=0), rows, put_lat)

    settle(adj.at[pl.ds(0, 2)], load_sem.at[6 + len(groups)])

    def edge_piece(p):
        settle(recv_s.at[p], recv_sem.at[2 + p])
        edge(p)

    middle = order[:-2]
    cut = (len(middle) + 1) // 2
    for p in middle[:cut]:
        edge_piece(p)
    for n, (a, b) in enumerate(lat_groups):
        first_arrives(n)
        lax.fori_loop((a - 1) // 2, (b - 1) // 2, outer_pair, 0)
        lat_start(lambda side, n=n: side.second[n])
        if n == 0:
            for p in middle[cut:]:
                edge_piece(p)
    for p in order[-2:]:
        edge_piece(p)
    lat_start(lambda side: side.second[2])

    def back(r, chunk, lo, hi, west_t, east_t):
        c, s, w = chunk
        own = tt[r, c, 8 + lo : 8 + hi, 0:w]
        value = own + jnp.maximum(cxs[r + 1, c, lo:hi, 0:w], 0.0) * (east_t - own)
        value = value + jnp.minimum(cxs[r, c, lo:hi, 0:w], 0.0) * (own - west_t)
        value = value + jnp.maximum(cys[r, c, 8 + lo : 8 + hi, 0:w], 0.0) * (tt[r, c, 9 + lo : 9 + hi, 0:w] - own)
        value = value + jnp.minimum(cys[r, c, 7 + lo : 7 + hi, 0:w], 0.0) * (own - tt[r, c, 7 + lo : 7 + hi, 0:w])
        done[r, lo:hi, s : s + w] = value

    def back_row(segments):
        def one(r, carry):
            for chunk in chunks:
                c, _, w = chunk
                for lo, hi in segments:
                    near = [tt[r + d, c, 8 + lo : 8 + hi, 0:w] for d in (-1, 1)]
                    back(r, chunk, lo, hi, *near)
            return carry

        return one

    lax.fori_loop(1, rows - 1, back_row(inner), 0)
    for n, (a, b) in enumerate(lat_groups):
        second_arrives(n)
        lax.fori_loop(a, b, back_row(outer), 0)
    second_arrives(2)
    for p in order:
        settle(recv_t.at[p], recv_sem.at[2 + tiles + p])
        lo, hi = TILE * p, TILE * p + TILE
        for chunk in chunks:
            c, _, w = chunk
            back(0, chunk, lo, hi, unpack(plan_neg, chunk, recv_t.at[p, 0]), tt[1, c, 8 + lo : 8 + hi, 0:w])
            back(rows - 1, chunk, lo, hi, tt[rows - 2, c, 8 + lo : 8 + hi, 0:w], unpack(plan_pos, chunk, recv_t.at[p, 1]))

    for n, ref in enumerate((face_f, face_i, send_s, send_t)):
        settle(ref, send_sem.at[n])
    for side, edge_rim in zip(lat_all, (rim.at[1], rim.at[0])):
        @pl.when(side.there)
        def _(side=side, edge_rim=edge_rim):
            for copy in side.small:
                copy.wait_send()
            settle(edge_rim, send_sem.at[side.out + 2])
            settle(tt.at[:, :, pl.ds(side.own, 1)], send_sem.at[side.out + 3])


def keep(array):
    return pltpu.with_memory_space_constraint(array, pltpu.HBM)


def round_up(value, step):
    return (value + step - 1) // step * step


def body(nx, ny, spectrum, adjoint_in, cx, cy, wx, wy, land, ice, speed, growth, diss):
    rows, cells, bins = spectrum.shape
    freqs = speed.shape[0]
    angles = 2.0 * math.pi / DIRS * (np.arange(DIRS) + 0.5)
    cosine, sine = (np.repeat(f(angles), freqs) for f in (np.cos, np.sin))
    plan_pos, plan_neg = slot_plan(cosine > -CERTAIN), slot_plan(cosine < CERTAIN)
    slots = max(len(plan_pos), len(plan_neg))
    many = round_up(freqs, 16)
    hot = (np.arange(many)[:, None] == np.arange(bins)[None] % freqs).astype(np.float32)
    consts = np.concatenate([hot, np.tile(cosine, (TILE, 1)), np.tile(sine, (TILE, 1))]).astype(np.float32)
    tiles, width = cells // TILE, -(-bins // LANES)
    tall = round_up(rows + 2, 8)
    first = 1 + 2 * ((rows - 2) // 4 + 1)
    lat_groups = ((1, first), (first, rows - 1))
    f32 = jnp.float32
    dma = pltpu.SemaphoreType.DMA
    vmem = lambda *shape: pltpu.VMEM(shape, f32)
    return pl.pallas_call(
        functools.partial(kernel, nx, ny, plan_pos, plan_neg, lat_groups),
        out_shape=jax.ShapeDtypeStruct((rows, cells, bins), f32),
        in_specs=[HBM] * 12,
        out_specs=VMEM,
        scratch_shapes=[
            vmem(2, rows, cells, bins),
            vmem(2, rows, 1, bins),
            vmem(2, rows, 1, bins),
            vmem(rows, width, cells + 16, LANES),
            vmem(rows + 1, width, cells, LANES),
            vmem(2, width, cells, LANES),
            vmem(rows, width, cells + 8, LANES),
            vmem(5, width, TILE, LANES),
            vmem(rows + 1, cells, LANES),
            vmem(rows + 1, cells, LANES),
            vmem(rows, cells + TILE, LANES),
            vmem(rows, cells + TILE, LANES),
            vmem(rows, cells, LANES),
            vmem(rows, cells, LANES),
            vmem(rows, cells, LANES),
            vmem(tiles, 2, slots, TILE, LANES),
            vmem(tiles, 2, slots, TILE, LANES),
            vmem(tiles, 2, slots, TILE, LANES),
            vmem(tiles, 2, slots, TILE, LANES),
            vmem(4, rows, cells),
            pltpu.VMEM((2, rows, cells), jnp.int32),
            vmem(2, rows, cells),
            pltpu.VMEM((2, rows, cells), jnp.int32),
            vmem(2, TILE, cells),
            pltpu.VMEM((2, TILE, cells), jnp.int32),
            vmem(3, 1, freqs),
            vmem(many + 2 * TILE, bins),
            vmem(3 * TILE, many),
            vmem(11, tall, LANES),
            vmem(8, width, cells + 8, LANES),
            dma((11,)),
            dma((12,)),
            dma((2 + 2 * tiles + 14,)),
        ],
        compiler_params=pltpu.CompilerParams(
            collective_id=0, has_side_effects=True, vmem_limit_bytes=40 * 2**20
        ),
        name="step",
    )(*map(keep, (spectrum, adjoint_in, cx, cy, wx, wy, land, ice)),
      *map(keep, (speed.reshape(1, -1), growth.reshape(1, -1), diss.reshape(1, -1), jnp.asarray(consts))))


def solution(mesh):
    grid = P("gx", "gy")
    field = P("gx", "gy", None)
    return jax.shard_map(
        functools.partial(body, mesh.shape["gx"], mesh.shape["gy"]),
        mesh=mesh,
        in_specs=(field, field) + (grid,) * 6 + (P(), P(), P()),
        out_specs=field,
        check_vma=False,
    )
```

```python
import functools
import math
from types import SimpleNamespace

import jax
import jax.numpy as jnp
import numpy as np
from jax import lax
from jax.experimental import pallas as pl
from jax.experimental.pallas import tpu as pltpu
from jax.sharding import PartitionSpec as P

DIRS = 36
LANES = 128
TILE = 8
CERTAIN = 0.81
HBM = pl.BlockSpec(memory_space=pltpu.HBM)
VMEM = pl.BlockSpec(memory_space=pltpu.VMEM)
MESH = pl.DeviceIdType.MESH


def lane_chunks(bins):
    return [(c, s, min(LANES, bins - s)) for c, s in enumerate(range(0, bins, LANES))]


def slot_plan(need):
    parts = []
    for c, s, w in lane_chunks(len(need)):
        lane = 0
        while lane < w:
            if not need[s + lane]:
                lane += 1
                continue
            first = lane
            while lane < w and need[s + lane]:
                lane += 1
            parts.append((c, first, lane, w))
    parts.sort(key=lambda p: (p[3] == LANES, p[1] - p[2]))
    slots, used = [], []
    for c, first, last, w in parts:
        size = last - first
        for n, busy in enumerate(used):
            if not busy[first:last].any():
                shift = 0
            elif w == LANES:
                starts = [k for k in range(LANES - size + 1) if not busy[k : k + size].any()]
                if not starts:
                    continue
                shift = starts[0] - first
            else:
                continue
            busy[first + shift : last + shift] = True
            slots[n].append((c, first, last, shift % LANES))
            break
        else:
            busy = np.zeros(LANES, bool)
            busy[first:last] = True
            used.append(busy)
            slots.append([(c, first, last, 0)])
    return slots


def repeat(value, count):
    return value if count == 1 else jnp.concatenate([value] * count, axis=0)


def between(first, last):
    lane = lax.broadcasted_iota(jnp.int32, (TILE, LANES), 1)
    return jnp.logical_and(lane >= first, lane < last)


def pack(plan, chunks, load, out):
    for n, parts in enumerate(plan):
        value, late = None, None
        for c, first, last, shift in parts:
            w = chunks[c][2]
            if w < LANES:
                late = (c, w)
                continue
            part = load(c)
            if shift:
                part = pltpu.roll(part, shift, axis=1)
            begin = (first + shift) % LANES
            value = part if value is None else jnp.where(between(begin, begin + last - first), part, value)
        if value is not None:
            out[n] = value
        if late is not None:
            out[n, :, 0 : late[1]] = load(late[0])


def unpack(plan, chunk, slots):
    c, _, w = chunk
    value = jnp.zeros((TILE, w), jnp.float32)
    for n, parts in enumerate(plan):
        for chunk_of, first, last, shift in parts:
            if chunk_of != c:
                continue
            if w < LANES:
                part = slots[n, :, 0:w]
                if last - first < w:
                    part = jnp.where(between(first, last)[:, 0:w], part, 0.0)
                value = part
                continue
            part = slots[n]
            if shift:
                part = pltpu.roll(part, LANES - shift, axis=1)
            value = part if last - first == LANES else jnp.where(between(first, last), part, value)
    return value


def split3(value):
    high = value.astype(jnp.bfloat16).astype(jnp.float32)
    rest = value - high
    mid = rest.astype(jnp.bfloat16).astype(jnp.float32)
    return [high, mid, rest - mid]


def kernel(
    nx, ny, plan_pos, plan_neg,
    spectrum, adjoint, cx_h, cy_h, wx_h, wy_h, land_h, ice_h, speed_h, growth_h, diss_h, consts_h,
    done,
    both, rim, own_c, halo_c, adj_c, part_c, face_c, mine_c, next_c, cst, tt, cxs, fxs, cys, tab, opx, odx, opy, ody, wxs, wys, seas,
    send_s, recv_s, send_t, recv_t, mine_f, mine_i, near_f, near_i, face_f, face_i, coeffs, consts, params, ext, bufs, load_sem, send_sem, recv_sem,
):
    gx, gy = lax.axis_index("gx"), lax.axis_index("gy")
    rows, cells, bins = adjoint.shape
    east, west = lax.rem(gx + 1, nx), lax.rem(gx + nx - 1, nx)
    has_north, has_south = gy < ny - 1, gy > 0
    chunks = lane_chunks(bins)
    tiles = cells // TILE
    f32 = jnp.float32
    sp, adj = both.at[0], both.at[1]

    cx, cy, wx, wy = (mine_f.at[m] for m in range(4))
    land, ice = (mine_i.at[m] for m in range(2))
    speed, growth, diss = (coeffs.at[m] for m in range(3))
    pairs = (rows - 2) // 2
    bounds = [1, 4, 10, 16, rows - 1]
    local = lambda src, dst, n: pltpu.make_async_copy(src, dst, load_sem.at[n])
    ends = [local(spectrum.at[r], sp.at[r], 0) for r in (0, rows - 1)]
    small = [
        local(src, dst, n)
        for src, dst, n in (
            (cx_h, cx, 1), (cy_h, cy, 1), (wx_h, wx, 1), (wy_h, wy, 1), (land_h, land, 2), (ice_h, ice, 2),
            (speed_h, speed, 3), (growth_h, growth, 3), (diss_h, diss, 3), (consts_h, consts, 4),
        )
    ]
    rims = [
        local(spectrum.at[:, pl.ds(0, 1), :], rim.at[0], 5),
        local(spectrum.at[:, pl.ds(cells - 1, 1), :], rim.at[1], 5),
    ]
    groups = []
    for n, (a, b) in enumerate(zip(bounds[:-1], bounds[1:])):
        groups.append(
            [local(src.at[pl.ds(a, b - a)], dst.at[pl.ds(a, b - a)], 6 + n) for src, dst in ((spectrum, sp), (adjoint, adj))]
        )
    last_adj = [local(adjoint.at[r], adj.at[r], 6 + len(groups)) for r in (0, rows - 1)]
    for copy in ends + small + rims:
        copy.start()

    barrier = pltpu.get_barrier_semaphore()
    for where in (east, west):
        pl.semaphore_signal(barrier, inc=1, device_id={"gx": where}, device_id_type=MESH)

    @pl.when(has_north)
    def _():
        pl.semaphore_signal(barrier, inc=1, device_id={"gy": gy + 1}, device_id_type=MESH)

    @pl.when(has_south)
    def _():
        pl.semaphore_signal(barrier, inc=1, device_id={"gy": gy - 1}, device_id_type=MESH)

    for group in groups:
        for copy in group:
            copy.start()
    for copy in last_adj:
        copy.start()

    def far(src, dst, out, n, axis, where):
        return pltpu.make_async_remote_copy(
            src_ref=src, dst_ref=dst, send_sem=send_sem.at[out], recv_sem=recv_sem.at[n],
            device_id={axis: where}, device_id_type=MESH,
        )

    def settle(ref, sem):
        pltpu.make_async_copy(ref, ref, sem).wait()

    order = list(range(1, tiles - 1)) + [0, tiles - 1]
    ahead = []
    for m, (src, dst) in enumerate(((cx, face_f), (land, face_i))):
        ahead.append(far(src.at[pl.ds(rows - TILE, TILE)], dst.at[0], m, m, "gx", east))
        ahead.append(far(src.at[pl.ds(0, TILE)], dst.at[1], m, m, "gx", west))
    lon_s, lon_t = (
        [[far(src.at[p, d], dst.at[p, d], 2 + m, 2 + m * tiles + p, "gx", (east, west)[d]) for d in range(2)] for p in range(tiles)]
        for m, (src, dst) in enumerate(((send_s, recv_s), (send_t, recv_t)))
    )
    tops = rows // TILE
    span = lambda g: pl.ds(TILE * g, TILE)
    lat_all = []
    for d, (where, there, back_there) in enumerate(((gy + 1, has_north, has_south), (gy - 1, has_south, has_north))):
        sem = 2 + 2 * tiles + (2 + 2 * tops) * d
        away = lambda src, dst, out, n, where=where, d=d, sem=sem: far(src, dst, 4 + 4 * d + out, sem + n, "gy", where)
        lat_all.append(SimpleNamespace(
            there=there, back_there=back_there, out=4 + 4 * d,
            small=[away(cy, near_f.at[d], 0, 0), away(land, near_i.at[d], 1, 1)],
            first=[away(own_c.at[1 - d, :, span(g)], halo_c.at[d, :, span(g)], 2, 2 + g) for g in range(tops)],
            second=[away(mine_c.at[1 - d, :, span(g)], next_c.at[d, :, span(g)], 3, 2 + tops + g) for g in range(tops)],
        ))

    def lat_start(pick):
        for side in lat_all:
            @pl.when(side.there)
            def _(side=side):
                for copy in pick(side):
                    copy.start()

    def lat_arrive(pick):
        for side in lat_all:
            @pl.when(side.back_there)
            def _(side=side):
                pick(side)

    def first_arrives(n):
        lat_arrive(lambda side: side.first[n].wait_recv())

    def second_arrives(n):
        lat_arrive(lambda side: side.second[n].wait_recv())

    settle(sp.at[pl.ds(0, 2)], load_sem.at[0])
    for p in range(tiles):
        for d, (row, plan) in enumerate(((rows - 1, plan_pos), (0, plan_neg))):
            load = lambda c, row=row, p=p: sp[row, TILE * p : TILE * p + TILE, chunks[c][1] : chunks[c][1] + chunks[c][2]]
            pack(plan, chunks, load, send_s.at[p, d])
    for n, ref in enumerate((mine_f, mine_i, coeffs, consts, rim)):
        settle(ref, load_sem.at[1 + n])

    nil = jnp.zeros((1, LANES), f32)

    def prepare(r, carry):
        for c, s, w in chunks:
            for d in range(2):
                own_c[d, c, pl.ds(r, 1), 0:w] = rim[d, r, :, s : s + w]
            tt[r, c, 7:8] = nil
            tt[r, c, 8 + cells : 9 + cells] = nil
            cys[r, c, 7:8] = nil
        return carry

    lax.fori_loop(0, rows, prepare, 0)
    for q in range(2):
        for c, _, _ in chunks:
            bufs[4 * q, c, cells : cells + 1] = nil
            bufs[4 * q + 1, c, 7:8] = nil
    freqs = coeffs.shape[2]
    params[...] = jnp.zeros(params.shape, f32)
    for m, ref in enumerate((speed, growth, diss)):
        params[TILE * m : TILE * m + TILE, 0:freqs] = jnp.broadcast_to(ref[...], (TILE, freqs))
    many = params.shape[1]
    hot = consts[0:many].astype(jnp.bfloat16)
    by_bin = sum(
        jnp.dot(part.astype(jnp.bfloat16), hot, preferred_element_type=f32) for part in split3(params[...])
    )
    cosine, sine = consts[many : many + TILE], consts[many + TILE : many + 2 * TILE]
    for c, s, w in chunks:
        cs = slice(s, s + w)
        tab[0, c, :, 0:w] = by_bin[0:TILE, cs] * cosine[:, cs]
        tab[1, c, :, 0:w] = by_bin[0:TILE, cs] * sine[:, cs]
        tab[2, c, :, 0:w] = by_bin[TILE : 2 * TILE, cs] * cosine[:, cs]
        tab[3, c, :, 0:w] = by_bin[TILE : 2 * TILE, cs] * sine[:, cs]
        tab[4, c, :, 0:w] = by_bin[2 * TILE : 3 * TILE, cs]

    sub = lax.broadcasted_iota(jnp.int32, (LANES, 2 * LANES), 0)
    half = (lax.broadcasted_iota(jnp.int32, (LANES, 2 * LANES), 1) >= LANES).astype(jnp.int32)
    row_of = jnp.where(sub < rows, sub, jnp.where(sub < 2 * rows, sub - rows, jnp.where(sub < 3 * rows, sub - 2 * rows, -2)))
    row_of = row_of - half

    def turned(field):
        stack = split3(field)
        stack.append(jnp.zeros((LANES - 3 * rows, LANES), f32))
        return jnp.concatenate(stack, axis=0).T

    def spread(lhs, count, put):
        lhs = lhs.astype(jnp.bfloat16)
        for n in range(count // 2):
            pick = jnp.where(row_of == 2 * n, 1.0, 0.0).astype(jnp.bfloat16)
            out = jnp.dot(lhs, pick, preferred_element_type=f32)
            put(2 * n, out[:, 0:LANES])
            put(2 * n + 1, out[:, LANES:])

    sea_of = lambda mask: (1 - mask).astype(f32)
    ext[...] = jnp.zeros(ext.shape, f32)
    ice_free = sea_of(ice[...])
    ext[0, 1 : rows + 1, 0:cells] = cx[...]
    ext[1, 1 : rows + 1, 0:cells] = sea_of(land[...])
    ext[2, 0:rows, 0:cells] = cy[...]
    ext[3, 0:rows, 0:cells] = sea_of(land[...])
    windy = ice_free * sea_of(land[...])
    ext[8, 0:rows, 0:cells] = wx[...] * windy
    ext[9, 0:rows, 0:cells] = wy[...] * windy
    lane = lax.broadcasted_iota(jnp.int32, (rows, LANES), 1)
    sea, drift = ext[3, 0:rows], ext[2, 0:rows]
    opened_x = ext[1, 0:rows] * ext[1, 1 : rows + 1]
    ahead_of = lambda value: pltpu.roll(value, LANES - 1, axis=1)
    opened_y = sea * ahead_of(sea)
    fields = [
        opened_x, opened_x * (0.5 * (ext[0, 0:rows] + ext[0, 1 : rows + 1])),
        opened_y, opened_y * (0.5 * (drift + ahead_of(drift))),
        ext[8, 0:rows], ext[9, 0:rows], sea,
    ]
    homes = (opx, odx, opy, ody, wxs, wys, seas)

    def put_all(i, block):
        for k, home in enumerate(homes):
            home[i, 0:cells] = block[k * cells : (k + 1) * cells]

    spread(jnp.concatenate([turned(f)[0:cells] for f in fields], axis=0), rows, put_all)

    for m, field in enumerate((ext[8, 0:rows], ext[9, 0:rows], sea)):
        for d, cell in enumerate((0, cells - 1)):
            cst[d, 2 + m] = jnp.broadcast_to(field[:, cell : cell + 1], (rows, LANES))
    for d, there in enumerate((has_south, has_north)):
        @pl.when(jnp.logical_not(there))
        def _(d=d):
            halo_c[d] = jnp.zeros(halo_c.shape[1:], f32)
            next_c[d] = jnp.zeros(next_c.shape[1:], f32)

    def lat_part(buf, r, chunk, lo, own, fields, first, last, ends):
        c, s, w = chunk
        hi = lo + TILE
        sine_row = tab[1, c, :, 0:w]
        if first:
            buf.near[c, lo:hi, 0:w] = own
        if not last:
            buf.near[c, hi : hi + TILE, 0:w] = sp[r, hi : hi + TILE, s : s + w]
        elif hi < cells:
            buf.near[c, hi : hi + 1, 0:w] = sp[r, hi : hi + 1, s : s + w]
        elif ends:
            buf.near[c, hi : hi + 1, 0:w] = halo_c[1, c, r : r + 1, 0:w]
        upper = buf.near[c, lo + 1 : hi + 1, 0:w]
        courant = fields[0][:, 0:w] * sine_row + fields[1][:, 0:w]
        cys[r, c, 8 + lo : 8 + hi, 0:w] = courant
        fy = courant * jnp.where(courant > 0, own, upper)
        buf.flux[c, 8 + lo : 8 + hi, 0:w] = fy
        if first and (lo or ends):
            if lo:
                low = opy[r, lo - 1 : lo, 0:w] * sine_row[0:1] + ody[r, lo - 1 : lo, 0:w]
                below = sp[r, lo - 1 : lo, s : s + w]
            else:
                low = cst[0, 0, r : r + 1, 0:w] * sine_row[0:1] + cst[0, 1, r : r + 1, 0:w]
                below = halo_c[0, c, r : r + 1, 0:w]
                cys[r, c, 7 + lo : 8 + lo, 0:w] = low
            buf.flux[c, 7 + lo : 8 + lo, 0:w] = low * jnp.where(low > 0, below, own[0:1])
        return fy - buf.flux[c, 7 + lo : 7 + hi, 0:w]

    def lon_cells(f, lo):
        return opx[f, lo : lo + TILE], odx[f, lo : lo + TILE]

    def lon_speed(f, chunk, lo, fields):
        c, _, w = chunk
        speed = fields[0][:, 0:w] * tab[0, c, :, 0:w] + fields[1][:, 0:w]
        cxs[f, c, lo : lo + TILE, 0:w] = speed
        return speed

    def upwind(speed, here, there):
        return speed * jnp.where(speed > 0, here, there)

    def gather(totals, rest):
        value = jnp.sum(totals, axis=1, keepdims=True)
        return value if rest is None else value + rest

    def mean(sums):
        return jnp.broadcast_to(gather(*sums) * (1.0 / bins), (TILE, LANES))

    def weigh(chunk, advected, incoming, energy, wind_x, wind_y, open_sea, sums):
        c, _, w = chunk
        blow = wind_x[:, 0:w] * tab[2, c, :, 0:w] + wind_y[:, 0:w] * tab[3, c, :, 0:w]
        gain = open_sea[:, 0:w] + jnp.maximum(blow, 0.0)
        scaled = tab[4, c, :, 0:w] * advected
        damp = 1.0 + energy[:, 0:w] * scaled
        weighted = incoming * gain / (damp * damp)
        return weighted, add_up(chunk, weighted * scaled * advected, *sums)

    def add_up(chunk, value, total, rest):
        if chunk[2] == LANES:
            return total + value, rest
        return total, jnp.sum(value, axis=1, keepdims=True)

    none = (jnp.zeros((TILE, LANES), f32), None)
    slots = [SimpleNamespace(near=bufs.at[4 * q], flux=bufs.at[4 * q + 1], moved=bufs.at[4 * q + 2], weight=bufs.at[4 * q + 3]) for q in range(4)]

    def source(bufs_of, rows_of, lo, sums):
        hi = lo + TILE
        energy = [mean(each) for each in sums]
        sums = [none for _ in sums]
        fields = [(wxs[r, lo:hi], wys[r, lo:hi], seas[r, lo:hi]) for r in rows_of]
        for chunk in chunks:
            c, s, w = chunk
            for q, (buf, r) in enumerate(zip(bufs_of, rows_of)):
                weighted, sums[q] = weigh(chunk, buf.moved[c, lo:hi, 0:w], adj[r, lo:hi, s : s + w], energy[q], *fields[q], sums[q])
                buf.weight[c, lo:hi, 0:w] = weighted
        yield
        coupling = [mean(each) for each in sums]
        for c, s, w in chunks:
            for q, (buf, r) in enumerate(zip(bufs_of, rows_of)):
                tt[r, c, 8 + lo : 8 + hi, 0:w] = buf.weight[c, lo:hi, 0:w] - coupling[q][:, 0:w]
        yield

    def stagger(first, jobs):
        running = []
        for step in range(len(jobs) + 2):
            if step < len(jobs):
                running.append(first(jobs[step]))
            for n in (step - 1, step - 2):
                if 0 <= n < len(jobs):
                    next(running[n])

    def row_pair(r, chosen):
        def advance(a):
            lo, hi = TILE * a, TILE * a + TILE
            first, last = a - 1 not in chosen, a + 1 not in chosen
            sums = [none, none]
            lon = [lon_cells(r + q + 1, lo) for q in range(2)]
            lat = [(opy[r + q, lo:hi], ody[r + q, lo:hi]) for q in range(2)]
            for chunk in chunks:
                c, s, w = chunk
                own = [sp[r + q, lo:hi, s : s + w] for q in range(3)]
                flux_west = fxs[0, c, lo:hi, 0:w]
                for q in range(2):
                    buf = slots[q]
                    flux = upwind(lon_speed(r + q + 1, chunk, lo, lon[q]), own[q], own[q + 1])
                    if q:
                        fxs[0, c, lo:hi, 0:w] = flux
                    moved = own[q] - (flux - flux_west) - lat_part(buf, r + q, chunk, lo, own[q], lat[q], first, last, False)
                    flux_west = flux
                    for d, cell in enumerate((0, cells - 1)):
                        if cell // TILE == a:
                            part_c[d, c, pl.ds(r + q, 1), 0:w] = moved[cell - lo : cell - lo + 1]
                            adj_c[d, c, pl.ds(r + q, 1), 0:w] = adj[r + q, cell : cell + 1, s : s + w]
                    buf.moved[c, lo:hi, 0:w] = moved
                    sums[q] = add_up(chunk, moved, *sums[q])
            return source(slots[0:2], (r, r + 1), lo, sums)

        stagger(advance, chosen)

    def edge(pieces):
        def advance(p):
            lo, hi = TILE * p, TILE * p + TILE
            sums = [none, none]
            lon = [lon_cells(f, lo) for f in (0, rows - 1, rows)]
            lat = [(opy[r, lo:hi], ody[r, lo:hi]) for r in (0, rows - 1)]
            for chunk in chunks:
                c, s, w = chunk
                for q, r in enumerate((0, rows - 1)):
                    own = sp[r, lo:hi, s : s + w]
                    if q == 0:
                        flux_west = upwind(lon_speed(0, chunk, lo, lon[0]), unpack(plan_pos, chunk, recv_s.at[p, 0]), own)
                        flux = fxs[1, c, lo:hi, 0:w]
                    else:
                        before = lon_speed(rows - 1, chunk, lo, lon[1])
                        flux_west = upwind(before, sp[rows - 2, lo:hi, s : s + w], own)
                        flux = upwind(lon_speed(rows, chunk, lo, lon[2]), own, unpack(plan_neg, chunk, recv_s.at[p, 1]))
                    moved = own - (flux - flux_west) - lat_part(slots[2 + q], r, chunk, lo, own, lat[q], p == 0, p == tiles - 1, True)
                    slots[2 + q].moved[c, lo:hi, 0:w] = moved
                    sums[q] = add_up(chunk, moved, *sums[q])
            return source(slots[2:4], (0, rows - 1), lo, sums)

        for p in pieces:
            settle(recv_s.at[p], recv_sem.at[2 + p])
        stagger(advance, pieces)
        for p in pieces:
            lo, hi = TILE * p, TILE * p + TILE
            for d, (row, plan) in enumerate(((rows - 1, plan_neg), (0, plan_pos))):
                pack(plan, chunks, lambda c, row=row: tt[row, c, 8 + lo : 8 + hi, 0 : chunks[c][2]], send_t.at[p, d])
            for copy in lon_t[p]:
                copy.start()

    def ends_of(groups_of):
        jobs = [(g, d) for g in groups_of for d in range(2)]

        def advance(job):
            g, d = job
            at, sums = slice(TILE * g, TILE * g + TILE), none
            for chunk in chunks:
                c, _, w = chunk
                courant = cst[d, 0, at, 0:w] * tab[1, c, :, 0:w] + cst[d, 1, at, 0:w]
                face_c[d, c, at, 0:w] = courant
                own, halo = own_c[d, c, at, 0:w], halo_c[d, c, at, 0:w]
                flux = upwind(courant, halo, own) if d == 0 else -upwind(courant, own, halo)
                moved = part_c[d, c, at, 0:w] + flux
                part_c[d, c, at, 0:w] = moved
                sums = add_up(chunk, moved, *sums)
            return finish(g, d, sums)

        def finish(g, d, sums):
            at = slice(TILE * g, TILE * g + TILE)
            energy, sums = mean(sums), none
            for chunk in chunks:
                c, _, w = chunk
                mine_c[d, c, at, 0:w], sums = weigh(
                    chunk, part_c[d, c, at, 0:w], adj_c[d, c, at, 0:w], energy, cst[d, 2, at], cst[d, 3, at], cst[d, 4, at], sums
                )
            yield
            coupling = mean(sums)
            for c, _, w in chunks:
                mine_c[d, c, at, 0:w] = mine_c[d, c, at, 0:w] - coupling[:, 0:w]
            yield

        stagger(advance, jobs)
        for g in groups_of:
            for r in range(TILE * g, TILE * g + TILE):
                for c, _, w in chunks:
                    for d, cell in enumerate((0, cells - 1)):
                        if 0 < r < rows - 1:
                            tt[r, c, 8 + cell : 9 + cell, 0:w] = mine_c[d, c, r : r + 1, 0:w]

    def send_ends(g):
        for r in (0, rows - 1):
            if r // TILE == g:
                for c, _, w in chunks:
                    for d, cell in enumerate((0, cells - 1)):
                        mine_c[d, c, r : r + 1, 0:w] = tt[r, c, 8 + cell : 9 + cell, 0:w]
        lat_start(lambda side: [side.second[g]])

    def wait_group(n):
        settle(both.at[:, pl.ds(bounds[n], bounds[n + 1] - bounds[n])], load_sem.at[6 + n])

    wait_group(0)
    for lo in range(0, cells, TILE):
        lon = lon_cells(1, lo)
        for chunk in chunks:
            c, s, w = chunk
            flux = upwind(lon_speed(1, chunk, lo, lon), sp[0, lo : lo + TILE, s : s + w], sp[1, lo : lo + TILE, s : s + w])
            for m in range(2):
                fxs[m, c, lo : lo + TILE, 0:w] = flux

    pl.semaphore_wait(barrier, 2 + has_north.astype(jnp.int32) + has_south.astype(jnp.int32))
    for copy in ahead:
        copy.start()
    lat_start(lambda side: side.small)
    for p in order:
        for copy in lon_s[p]:
            copy.start()
    lat_start(lambda side: side.first)

    firsts = [next(k for k in range(pairs + 1) if 3 + 2 * k >= b) for b in bounds[1:-1]]

    def halo_faces():
        for m, ref in enumerate((face_f, face_i)):
            settle(ref, recv_sem.at[m])
        lat_arrive(lambda side: [copy.wait_recv() for copy in side.small])
        ext[0, 0:1, 0:cells] = face_f[0, TILE - 1 : TILE]
        ext[0, rows + 1 : rows + 2, 0:cells] = face_f[1, 0:1]
        ext[1, 0:1, 0:cells] = sea_of(face_i[0, TILE - 1 : TILE])
        ext[1, rows + 1 : rows + 2, 0:cells] = sea_of(face_i[1, 0:1])
        ext[4, 0:rows, 0:cells] = near_f[0]
        ext[5, 0:rows, 0:cells] = sea_of(near_i[0])
        ext[6, 0:rows, 0:cells] = near_f[1]
        ext[7, 0:rows, 0:cells] = sea_of(near_i[1])
        for n, f in enumerate((0, rows)):
            opened = ext[1, f : f + 1] * ext[1, f + 1 : f + 2]
            ext[10, n : n + 1] = opened
            ext[10, n + 2 : n + 3] = opened * (0.5 * (ext[0, f : f + 1] + ext[0, f + 1 : f + 2]))

        def put_lon(i, block):
            (opx, odx)[i // 2][(0, rows)[i % 2], 0:cells] = block

        spread(turned(ext[10, 0:rows])[0:cells], 4, put_lon)

        def with_ends(own, south, north):
            mine = jnp.where(lane == cells, pltpu.roll(own, cells, axis=1), own)
            other = jnp.where(lane == cells - 1, pltpu.roll(north, cells - 1, axis=1), ahead_of(own))
            return mine, jnp.where(lane == cells, pltpu.roll(south, 1, axis=1), other)

        sea_a, sea_b = with_ends(ext[3, 0:rows], ext[5, 0:rows], ext[7, 0:rows])
        cy_a, cy_b = with_ends(ext[2, 0:rows], ext[4, 0:rows], ext[6, 0:rows])
        closed = jnp.logical_or(
            jnp.logical_and(lane == cells, jnp.logical_not(has_south)),
            jnp.logical_and(lane == cells - 1, jnp.logical_not(has_north)),
        )
        opened = jnp.where(closed, 0.0, sea_a * sea_b)
        drift = jnp.where(closed, 0.0, opened * (0.5 * (cy_a + cy_b)))
        for m, (field, home) in enumerate(((opened, opy), (drift, ody))):
            for d, face in enumerate((cells, cells - 1)):
                cst[d, m] = jnp.broadcast_to(field[:, face : face + 1], (rows, LANES))
            for r in (0, rows - 1):
                home[r, cells - 1 : cells] = cst[1, m, r : r + 1]
        settle(adj.at[pl.ds(0, 2)], load_sem.at[6 + len(groups)])
        for r in (0, rows - 1):
            for c, s, w in chunks:
                for d in range(2):
                    part_c[d, c, r : r + 1, 0:w] = nil[:, 0:w]
                    adj_c[d, c, r : r + 1, 0:w] = nil[:, 0:w]

    cut = pairs // 2 + 1
    every, outer, inner = list(range(tiles)), [0, tiles - 1], list(range(1, tiles - 1))

    def step(chosen):
        def one(k, carry):
            for n, first in enumerate(firsts):
                if chosen != inner:
                    @pl.when(k == first)
                    def _(n=n):
                        wait_group(n + 1)

            row_pair(1 + 2 * k, chosen)
            return carry

        return one

    lax.fori_loop(0, cut, step(every), 0)
    lax.fori_loop(cut, pairs, step(outer), 0)
    for n in range(len(firsts)):
        if firsts[n] >= pairs:
            wait_group(n + 1)
    halo_faces()
    for g in range(tops):
        first_arrives(g)
    edge(every)
    ends_of(range(tops))
    for g in range(tops):
        send_ends(g)
    lax.fori_loop(cut, pairs, step(inner), 0)

    def back(r, count, chunk, lo, west_t, east_t):
        c, s, w = chunk
        hi = lo + TILE
        own = [tt[r + q, c, 8 + lo : 8 + hi, 0:w] for q in range(count)]
        line = [west_t] + own + [east_t]
        steps = [line[q + 1] - line[q] for q in range(count + 1)]
        speeds = [cxs[r + q, c, lo:hi, 0:w] for q in range(count + 1)]
        for q in range(count):
            value = own[q] + jnp.maximum(speeds[q + 1], 0.0) * steps[q + 1]
            value = value + jnp.minimum(speeds[q], 0.0) * steps[q]
            value = value + jnp.maximum(cys[r + q, c, 8 + lo : 8 + hi, 0:w], 0.0) * (tt[r + q, c, 9 + lo : 9 + hi, 0:w] - own[q])
            value = value + jnp.minimum(cys[r + q, c, 7 + lo : 7 + hi, 0:w], 0.0) * (own[q] - tt[r + q, c, 7 + lo : 7 + hi, 0:w])
            done[r + q, lo:hi, s : s + w] = value

    def back_pair(k, carry):
        r = 1 + 2 * k
        for chunk in chunks:
            c, _, w = chunk
            for lo in range(0, cells, TILE):
                near = [tt[r + d, c, 8 + lo : 8 + lo + TILE, 0:w] for d in (-1, 2)]
                back(r, 2, chunk, lo, *near)
        return carry

    lax.fori_loop(0, pairs, back_pair, 0)
    for g in range(tops):
        second_arrives(g)
        rows_of = slice(TILE * g, TILE * g + TILE)
        for d in range(2):
            for c, _, w in chunks:
                courant = face_c[d, c, rows_of, 0:w]
                step = next_c[d, c, rows_of, 0:w] - mine_c[d, c, rows_of, 0:w]
                if d == 0:
                    part_c[d, c, rows_of, 0:w] = -jnp.minimum(courant, 0.0) * step
                else:
                    part_c[d, c, rows_of, 0:w] = jnp.maximum(courant, 0.0) * step
        for r in range(TILE * g, TILE * g + TILE):
            for c, s, w in chunks:
                for d, cell in enumerate((0, cells - 1)):
                    if 0 < r < rows - 1:
                        done[r, cell : cell + 1, s : s + w] = done[r, cell : cell + 1, s : s + w] + part_c[d, c, r : r + 1, 0:w]
                    else:
                        beyond = (7, 8 + cells)[d]
                        tt[r, c, beyond : beyond + 1, 0:w] = next_c[d, c, r : r + 1, 0:w]
    for p in order:
        settle(recv_t.at[p], recv_sem.at[2 + tiles + p])
        lo, hi = TILE * p, TILE * p + TILE
        for chunk in chunks:
            c, _, w = chunk
            back(0, 1, chunk, lo, unpack(plan_neg, chunk, recv_t.at[p, 0]), tt[1, c, 8 + lo : 8 + hi, 0:w])
            back(rows - 1, 1, chunk, lo, tt[rows - 2, c, 8 + lo : 8 + hi, 0:w], unpack(plan_pos, chunk, recv_t.at[p, 1]))

    for n, ref in enumerate((face_f, face_i, send_s, send_t)):
        settle(ref, send_sem.at[n])
    for d, side in enumerate(lat_all):
        @pl.when(side.there)
        def _(d=d, side=side):
            for copy in side.small:
                copy.wait_send()
            settle(own_c.at[1 - d], send_sem.at[side.out + 2])
            settle(mine_c.at[1 - d], send_sem.at[side.out + 3])


def keep(array):
    return pltpu.with_memory_space_constraint(array, pltpu.HBM)


def round_up(value, step):
    return (value + step - 1) // step * step


def body(nx, ny, spectrum, adjoint_in, cx, cy, wx, wy, land, ice, speed, growth, diss):
    rows, cells, bins = spectrum.shape
    freqs = speed.shape[0]
    angles = 2.0 * math.pi / DIRS * (np.arange(DIRS) + 0.5)
    cosine, sine = (np.repeat(f(angles), freqs) for f in (np.cos, np.sin))
    plan_pos, plan_neg = slot_plan(cosine > -CERTAIN), slot_plan(cosine < CERTAIN)
    slots = max(len(plan_pos), len(plan_neg))
    many = round_up(freqs, 16)
    hot = (np.arange(many)[:, None] == np.arange(bins)[None] % freqs).astype(np.float32)
    consts = np.concatenate([hot, np.tile(cosine, (TILE, 1)), np.tile(sine, (TILE, 1))]).astype(np.float32)
    tiles, width = cells // TILE, -(-bins // LANES)
    tall = round_up(rows + 2, 8)
    compact = pltpu.VMEM((2, width, rows, LANES), jnp.float32)
    f32 = jnp.float32
    dma = pltpu.SemaphoreType.DMA
    vmem = lambda *shape: pltpu.VMEM(shape, f32)
    return pl.pallas_call(
        functools.partial(kernel, nx, ny, plan_pos, plan_neg),
        out_shape=jax.ShapeDtypeStruct((rows, cells, bins), f32),
        in_specs=[HBM] * 12,
        out_specs=VMEM,
        scratch_shapes=[
            vmem(2, rows, cells, bins),
            vmem(2, rows, 1, bins),
            compact, compact, compact, compact, compact, compact, compact,
            vmem(2, 5, rows, LANES),
            vmem(rows, width, cells + 16, LANES),
            vmem(rows + 1, width, cells, LANES),
            vmem(2, width, cells, LANES),
            vmem(rows, width, cells + 8, LANES),
            vmem(5, width, TILE, LANES),
            vmem(rows + 1, cells, LANES),
            vmem(rows + 1, cells, LANES),
            vmem(rows, cells, LANES),
            vmem(rows, cells, LANES),
            vmem(rows, cells, LANES),
            vmem(rows, cells, LANES),
            vmem(rows, cells, LANES),
            vmem(tiles, 2, slots, TILE, LANES),
            vmem(tiles, 2, slots, TILE, LANES),
            vmem(tiles, 2, slots, TILE, LANES),
            vmem(tiles, 2, slots, TILE, LANES),
            vmem(4, rows, cells),
            pltpu.VMEM((2, rows, cells), jnp.int32),
            vmem(2, rows, cells),
            pltpu.VMEM((2, rows, cells), jnp.int32),
            vmem(2, TILE, cells),
            pltpu.VMEM((2, TILE, cells), jnp.int32),
            vmem(3, 1, freqs),
            vmem(many + 2 * TILE, bins),
            vmem(3 * TILE, many),
            vmem(11, tall, LANES),
            vmem(16, width, cells + 8, LANES),
            dma((11,)),
            dma((12,)),
            dma((2 + 2 * tiles + 4 + 4 * (rows // TILE),)),
        ],
        compiler_params=pltpu.CompilerParams(
            collective_id=0, has_side_effects=True, vmem_limit_bytes=40 * 2**20
        ),
        name="step",
    )(*map(keep, (spectrum, adjoint_in, cx, cy, wx, wy, land, ice)),
      *map(keep, (speed.reshape(1, -1), growth.reshape(1, -1), diss.reshape(1, -1), jnp.asarray(consts))))


def solution(mesh):
    grid = P("gx", "gy")
    field = P("gx", "gy", None)
    return jax.shard_map(
        functools.partial(body, mesh.shape["gx"], mesh.shape["gy"]),
        mesh=mesh,
        in_specs=(field, field) + (grid,) * 6 + (P(), P(), P()),
        out_specs=field,
        check_vma=False,
    )
```

```python
import functools
import math
from types import SimpleNamespace

import jax
import jax.numpy as jnp
import numpy as np
from jax import lax
from jax.experimental import pallas as pl
from jax.experimental.pallas import tpu as pltpu
from jax.sharding import PartitionSpec as P

DIRS = 36
LANES = 128
TILE = 8
CERTAIN = 0.81
HBM = pl.BlockSpec(memory_space=pltpu.HBM)
VMEM = pl.BlockSpec(memory_space=pltpu.VMEM)
MESH = pl.DeviceIdType.MESH


def lane_chunks(bins):
    return [(c, s, min(LANES, bins - s)) for c, s in enumerate(range(0, bins, LANES))]


def slot_plan(need):
    parts = []
    for c, s, w in lane_chunks(len(need)):
        lane = 0
        while lane < w:
            if not need[s + lane]:
                lane += 1
                continue
            first = lane
            while lane < w and need[s + lane]:
                lane += 1
            parts.append((c, first, lane, w))
    parts.sort(key=lambda p: (p[3] == LANES, p[1] - p[2]))
    slots, used = [], []
    for c, first, last, w in parts:
        size = last - first
        for n, busy in enumerate(used):
            if not busy[first:last].any():
                shift = 0
            elif w == LANES:
                starts = [k for k in range(LANES - size + 1) if not busy[k : k + size].any()]
                if not starts:
                    continue
                shift = starts[0] - first
            else:
                continue
            busy[first + shift : last + shift] = True
            slots[n].append((c, first, last, shift % LANES))
            break
        else:
            busy = np.zeros(LANES, bool)
            busy[first:last] = True
            used.append(busy)
            slots.append([(c, first, last, 0)])
    return slots


def repeat(value, count):
    return value if count == 1 else jnp.concatenate([value] * count, axis=0)


def between(first, last):
    lane = lax.broadcasted_iota(jnp.int32, (TILE, LANES), 1)
    return jnp.logical_and(lane >= first, lane < last)


def pack(plan, chunks, load, out):
    for n, parts in enumerate(plan):
        value, late = None, None
        for c, first, last, shift in parts:
            w = chunks[c][2]
            if w < LANES:
                late = (c, w)
                continue
            part = load(c)
            if shift:
                part = pltpu.roll(part, shift, axis=1)
            begin = (first + shift) % LANES
            value = part if value is None else jnp.where(between(begin, begin + last - first), part, value)
        if value is not None:
            out[n] = value
        if late is not None:
            out[n, :, 0 : late[1]] = load(late[0])


def unpack(plan, chunk, slots):
    c, _, w = chunk
    value = jnp.zeros((TILE, w), jnp.float32)
    for n, parts in enumerate(plan):
        for chunk_of, first, last, shift in parts:
            if chunk_of != c:
                continue
            if w < LANES:
                part = slots[n, :, 0:w]
                if last - first < w:
                    part = jnp.where(between(first, last)[:, 0:w], part, 0.0)
                value = part
                continue
            part = slots[n]
            if shift:
                part = pltpu.roll(part, LANES - shift, axis=1)
            value = part if last - first == LANES else jnp.where(between(first, last), part, value)
    return value


def split3(value):
    high = value.astype(jnp.bfloat16).astype(jnp.float32)
    rest = value - high
    mid = rest.astype(jnp.bfloat16).astype(jnp.float32)
    return [high, mid, rest - mid]


def kernel(
    nx, ny, plan_pos, plan_neg,
    spectrum, adjoint, cx_h, cy_h, wx_h, wy_h, land_h, ice_h, speed_h, growth_h, diss_h, consts_h,
    done,
    both, rim, own_c, halo_c, adj_c, part_c, face_c, mine_c, next_c, cst, tt, cxs, fxs, cys, tab, opx, odx, opy, ody, wxs, wys, seas,
    send_s, recv_s, send_t, recv_t, mine_f, mine_i, near_f, near_i, face_f, face_i, coeffs, consts, params, ext, bufs, load_sem, send_sem, recv_sem,
):
    gx, gy = lax.axis_index("gx"), lax.axis_index("gy")
    rows, cells, bins = adjoint.shape
    east, west = lax.rem(gx + 1, nx), lax.rem(gx + nx - 1, nx)
    has_north, has_south = gy < ny - 1, gy > 0
    chunks = lane_chunks(bins)
    tiles = cells // TILE
    f32 = jnp.float32
    sp, adj = both.at[0], both.at[1]

    cx, cy, wx, wy = (mine_f.at[m] for m in range(4))
    land, ice = (mine_i.at[m] for m in range(2))
    speed, growth, diss = (coeffs.at[m] for m in range(3))
    pairs = (rows - 2) // 2
    bounds = [1, 4, 10, 16, rows - 1]
    local = lambda src, dst, n: pltpu.make_async_copy(src, dst, load_sem.at[n])
    ends = [local(spectrum.at[r], sp.at[r], 0) for r in (0, rows - 1)]
    small = [
        local(src, dst, n)
        for src, dst, n in (
            (cx_h, cx, 1), (cy_h, cy, 1), (wx_h, wx, 1), (wy_h, wy, 1), (land_h, land, 2), (ice_h, ice, 2),
            (speed_h, speed, 3), (growth_h, growth, 3), (diss_h, diss, 3), (consts_h, consts, 4),
        )
    ]
    rims = [
        local(spectrum.at[:, pl.ds(0, 1), :], rim.at[0], 5),
        local(spectrum.at[:, pl.ds(cells - 1, 1), :], rim.at[1], 5),
    ]
    groups = []
    for n, (a, b) in enumerate(zip(bounds[:-1], bounds[1:])):
        groups.append(
            [local(src.at[pl.ds(a, b - a)], dst.at[pl.ds(a, b - a)], 6 + n) for src, dst in ((spectrum, sp), (adjoint, adj))]
        )
    last_adj = [local(adjoint.at[r], adj.at[r], 6 + len(groups)) for r in (0, rows - 1)]
    for copy in ends + small + rims:
        copy.start()

    barrier = pltpu.get_barrier_semaphore()
    for where in (east, west):
        pl.semaphore_signal(barrier, inc=1, device_id={"gx": where}, device_id_type=MESH)

    @pl.when(has_north)
    def _():
        pl.semaphore_signal(barrier, inc=1, device_id={"gy": gy + 1}, device_id_type=MESH)

    @pl.when(has_south)
    def _():
        pl.semaphore_signal(barrier, inc=1, device_id={"gy": gy - 1}, device_id_type=MESH)

    for group in groups:
        for copy in group:
            copy.start()
    for copy in last_adj:
        copy.start()

    def far(src, dst, out, n, axis, where):
        return pltpu.make_async_remote_copy(
            src_ref=src, dst_ref=dst, send_sem=send_sem.at[out], recv_sem=recv_sem.at[n],
            device_id={axis: where}, device_id_type=MESH,
        )

    def settle(ref, sem):
        pltpu.make_async_copy(ref, ref, sem).wait()

    order = list(range(1, tiles - 1)) + [0, tiles - 1]
    ahead = []
    for m, (src, dst) in enumerate(((cx, face_f), (land, face_i))):
        ahead.append(far(src.at[pl.ds(rows - TILE, TILE)], dst.at[0], m, m, "gx", east))
        ahead.append(far(src.at[pl.ds(0, TILE)], dst.at[1], m, m, "gx", west))
    lon_s, lon_t = (
        [[far(src.at[p, d], dst.at[p, d], 2 + m, 2 + m * tiles + p, "gx", (east, west)[d]) for d in range(2)] for p in range(tiles)]
        for m, (src, dst) in enumerate(((send_s, recv_s), (send_t, recv_t)))
    )
    tops = rows // TILE
    span = lambda g: pl.ds(TILE * g, TILE)
    lat_all = []
    for d, (where, there, back_there) in enumerate(((gy + 1, has_north, has_south), (gy - 1, has_south, has_north))):
        sem = 2 + 2 * tiles + (2 + 2 * tops) * d
        away = lambda src, dst, out, n, where=where, d=d, sem=sem: far(src, dst, 4 + 4 * d + out, sem + n, "gy", where)
        lat_all.append(SimpleNamespace(
            there=there, back_there=back_there, out=4 + 4 * d,
            small=[away(cy, near_f.at[d], 0, 0), away(land, near_i.at[d], 1, 1)],
            first=[away(own_c.at[1 - d, :, span(g)], halo_c.at[d, :, span(g)], 2, 2 + g) for g in range(tops)],
            second=[away(mine_c.at[1 - d, :, span(g)], next_c.at[d, :, span(g)], 3, 2 + tops + g) for g in range(tops)],
        ))

    def lat_start(pick):
        for side in lat_all:
            @pl.when(side.there)
            def _(side=side):
                for copy in pick(side):
                    copy.start()

    def lat_arrive(pick):
        for side in lat_all:
            @pl.when(side.back_there)
            def _(side=side):
                pick(side)

    def first_arrives(n):
        lat_arrive(lambda side: side.first[n].wait_recv())

    def second_arrives(n):
        lat_arrive(lambda side: side.second[n].wait_recv())

    settle(sp.at[pl.ds(0, 2)], load_sem.at[0])
    for p in range(tiles):
        for d, (row, plan) in enumerate(((rows - 1, plan_pos), (0, plan_neg))):
            load = lambda c, row=row, p=p: sp[row, TILE * p : TILE * p + TILE, chunks[c][1] : chunks[c][1] + chunks[c][2]]
            pack(plan, chunks, load, send_s.at[p, d])
    for n, ref in enumerate((mine_f, mine_i, coeffs, consts, rim)):
        settle(ref, load_sem.at[1 + n])

    nil = jnp.zeros((1, LANES), f32)

    def prepare(r, carry):
        for c, s, w in chunks:
            for d in range(2):
                own_c[d, c, pl.ds(r, 1), 0:w] = rim[d, r, :, s : s + w]
            tt[r, c, 7:8] = nil
            tt[r, c, 8 + cells : 9 + cells] = nil
            cys[r, c, 7:8] = nil
        return carry

    lax.fori_loop(0, rows, prepare, 0)
    for q in range(2):
        for c, _, _ in chunks:
            bufs[4 * q, c, cells : cells + 1] = nil
            bufs[4 * q + 1, c, 7:8] = nil
    freqs = coeffs.shape[2]
    params[...] = jnp.zeros(params.shape, f32)
    for m, ref in enumerate((speed, growth, diss)):
        params[TILE * m : TILE * m + TILE, 0:freqs] = jnp.broadcast_to(ref[...], (TILE, freqs))
    many = params.shape[1]
    hot = consts[0:many].astype(jnp.bfloat16)
    by_bin = sum(
        jnp.dot(part.astype(jnp.bfloat16), hot, preferred_element_type=f32) for part in split3(params[...])
    )
    cosine, sine = consts[many : many + TILE], consts[many + TILE : many + 2 * TILE]
    for c, s, w in chunks:
        cs = slice(s, s + w)
        tab[0, c, :, 0:w] = by_bin[0:TILE, cs] * cosine[:, cs]
        tab[1, c, :, 0:w] = by_bin[0:TILE, cs] * sine[:, cs]
        tab[2, c, :, 0:w] = by_bin[TILE : 2 * TILE, cs] * cosine[:, cs]
        tab[3, c, :, 0:w] = by_bin[TILE : 2 * TILE, cs] * sine[:, cs]
        tab[4, c, :, 0:w] = by_bin[2 * TILE : 3 * TILE, cs]

    sub = lax.broadcasted_iota(jnp.int32, (LANES, 2 * LANES), 0)
    half = (lax.broadcasted_iota(jnp.int32, (LANES, 2 * LANES), 1) >= LANES).astype(jnp.int32)
    row_of = jnp.where(sub < rows, sub, jnp.where(sub < 2 * rows, sub - rows, jnp.where(sub < 3 * rows, sub - 2 * rows, -2)))
    row_of = row_of - half

    def turned(field):
        stack = split3(field)
        stack.append(jnp.zeros((LANES - 3 * rows, LANES), f32))
        return jnp.concatenate(stack, axis=0).T

    def spread(lhs, count, put):
        lhs = lhs.astype(jnp.bfloat16)
        for n in range(count // 2):
            pick = jnp.where(row_of == 2 * n, 1.0, 0.0).astype(jnp.bfloat16)
            out = jnp.dot(lhs, pick, preferred_element_type=f32)
            put(2 * n, out[:, 0:LANES])
            put(2 * n + 1, out[:, LANES:])

    sea_of = lambda mask: (1 - mask).astype(f32)
    ext[...] = jnp.zeros(ext.shape, f32)
    ice_free = sea_of(ice[...])
    ext[0, 1 : rows + 1, 0:cells] = cx[...]
    ext[1, 1 : rows + 1, 0:cells] = sea_of(land[...])
    ext[2, 0:rows, 0:cells] = cy[...]
    ext[3, 0:rows, 0:cells] = sea_of(land[...])
    windy = ice_free * sea_of(land[...])
    ext[8, 0:rows, 0:cells] = wx[...] * windy
    ext[9, 0:rows, 0:cells] = wy[...] * windy
    lane = lax.broadcasted_iota(jnp.int32, (rows, LANES), 1)
    sea, drift = ext[3, 0:rows], ext[2, 0:rows]
    opened_x = ext[1, 0:rows] * ext[1, 1 : rows + 1]
    ahead_of = lambda value: pltpu.roll(value, LANES - 1, axis=1)
    opened_y = sea * ahead_of(sea)
    fields = [
        opened_x, opened_x * (0.5 * (ext[0, 0:rows] + ext[0, 1 : rows + 1])),
        opened_y, opened_y * (0.5 * (drift + ahead_of(drift))),
        ext[8, 0:rows], ext[9, 0:rows], sea,
    ]
    homes = (opx, odx, opy, ody, wxs, wys, seas)

    def put_all(i, block):
        for k, home in enumerate(homes):
            home[i, 0:cells] = block[k * cells : (k + 1) * cells]

    spread(jnp.concatenate([turned(f)[0:cells] for f in fields], axis=0), rows, put_all)

    for m, field in enumerate((ext[8, 0:rows], ext[9, 0:rows], sea)):
        for d, cell in enumerate((0, cells - 1)):
            cst[d, 2 + m] = jnp.broadcast_to(field[:, cell : cell + 1], (rows, LANES))
    for d, there in enumerate((has_south, has_north)):
        @pl.when(jnp.logical_not(there))
        def _(d=d):
            halo_c[d] = jnp.zeros(halo_c.shape[1:], f32)
            next_c[d] = jnp.zeros(next_c.shape[1:], f32)

    def lat_part(buf, r, chunk, lo, own, fields, first, last, ends):
        c, s, w = chunk
        hi = lo + TILE
        sine_row = tab[1, c, :, 0:w]
        if first:
            buf.near[c, lo:hi, 0:w] = own
        if not last:
            buf.near[c, hi : hi + TILE, 0:w] = sp[r, hi : hi + TILE, s : s + w]
        elif hi < cells:
            buf.near[c, hi : hi + 1, 0:w] = sp[r, hi : hi + 1, s : s + w]
        elif ends:
            buf.near[c, hi : hi + 1, 0:w] = halo_c[1, c, r : r + 1, 0:w]
        upper = buf.near[c, lo + 1 : hi + 1, 0:w]
        courant = fields[0][:, 0:w] * sine_row + fields[1][:, 0:w]
        cys[r, c, 8 + lo : 8 + hi, 0:w] = courant
        fy = courant * jnp.where(courant > 0, own, upper)
        buf.flux[c, 8 + lo : 8 + hi, 0:w] = fy
        if first and (lo or ends):
            if lo:
                low = opy[r, lo - 1 : lo, 0:w] * sine_row[0:1] + ody[r, lo - 1 : lo, 0:w]
                below = sp[r, lo - 1 : lo, s : s + w]
            else:
                low = cst[0, 0, r : r + 1, 0:w] * sine_row[0:1] + cst[0, 1, r : r + 1, 0:w]
                below = halo_c[0, c, r : r + 1, 0:w]
                cys[r, c, 7 + lo : 8 + lo, 0:w] = low
            buf.flux[c, 7 + lo : 8 + lo, 0:w] = low * jnp.where(low > 0, below, own[0:1])
        return fy - buf.flux[c, 7 + lo : 7 + hi, 0:w]

    def lon_cells(f, lo):
        return opx[f, lo : lo + TILE], odx[f, lo : lo + TILE]

    def lon_speed(f, chunk, lo, fields):
        c, _, w = chunk
        speed = fields[0][:, 0:w] * tab[0, c, :, 0:w] + fields[1][:, 0:w]
        cxs[f, c, lo : lo + TILE, 0:w] = speed
        return speed

    def upwind(speed, here, there):
        return speed * jnp.where(speed > 0, here, there)

    def gather(totals, rest):
        value = jnp.sum(totals, axis=1, keepdims=True)
        return value if rest is None else value + rest

    def mean(sums):
        return jnp.broadcast_to(gather(*sums) * (1.0 / bins), (TILE, LANES))

    def weigh(chunk, advected, incoming, energy, wind_x, wind_y, open_sea, sums):
        c, _, w = chunk
        blow = wind_x[:, 0:w] * tab[2, c, :, 0:w] + wind_y[:, 0:w] * tab[3, c, :, 0:w]
        gain = open_sea[:, 0:w] + jnp.maximum(blow, 0.0)
        scaled = tab[4, c, :, 0:w] * advected
        damp = 1.0 + energy[:, 0:w] * scaled
        weighted = incoming * gain / (damp * damp)
        return weighted, add_up(chunk, weighted * scaled * advected, *sums)

    def add_up(chunk, value, total, rest):
        if chunk[2] == LANES:
            return total + value, rest
        return total, jnp.sum(value, axis=1, keepdims=True)

    none = (jnp.zeros((TILE, LANES), f32), None)
    slots = [SimpleNamespace(near=bufs.at[4 * q], flux=bufs.at[4 * q + 1], moved=bufs.at[4 * q + 2], weight=bufs.at[4 * q + 3]) for q in range(4)]

    def source(bufs_of, rows_of, lo, sums):
        hi = lo + TILE
        energy = [mean(each) for each in sums]
        sums = [none for _ in sums]
        fields = [(wxs[r, lo:hi], wys[r, lo:hi], seas[r, lo:hi]) for r in rows_of]
        for chunk in chunks:
            c, s, w = chunk
            for q, (buf, r) in enumerate(zip(bufs_of, rows_of)):
                weighted, sums[q] = weigh(chunk, buf.moved[c, lo:hi, 0:w], adj[r, lo:hi, s : s + w], energy[q], *fields[q], sums[q])
                buf.weight[c, lo:hi, 0:w] = weighted
        yield
        coupling = [mean(each) for each in sums]
        for c, s, w in chunks:
            for q, (buf, r) in enumerate(zip(bufs_of, rows_of)):
                tt[r, c, 8 + lo : 8 + hi, 0:w] = buf.weight[c, lo:hi, 0:w] - coupling[q][:, 0:w]
        yield

    def stagger(first, jobs):
        running = []
        for step in range(len(jobs) + 2):
            if step < len(jobs):
                running.append(first(jobs[step]))
            for n in (step - 1, step - 2):
                if 0 <= n < len(jobs):
                    next(running[n])

    def row_pair(r, chosen):
        def advance(a):
            lo, hi = TILE * a, TILE * a + TILE
            first, last = a - 1 not in chosen, a + 1 not in chosen
            sums = [none, none]
            lon = [lon_cells(r + q + 1, lo) for q in range(2)]
            lat = [(opy[r + q, lo:hi], ody[r + q, lo:hi]) for q in range(2)]
            for chunk in chunks:
                c, s, w = chunk
                own = [sp[r + q, lo:hi, s : s + w] for q in range(3)]
                flux_west = fxs[0, c, lo:hi, 0:w]
                for q in range(2):
                    buf = slots[q]
                    flux = upwind(lon_speed(r + q + 1, chunk, lo, lon[q]), own[q], own[q + 1])
                    if q:
                        fxs[0, c, lo:hi, 0:w] = flux
                    moved = own[q] - (flux - flux_west) - lat_part(buf, r + q, chunk, lo, own[q], lat[q], first, last, False)
                    flux_west = flux
                    for d, cell in enumerate((0, cells - 1)):
                        if cell // TILE == a:
                            part_c[d, c, pl.ds(r + q, 1), 0:w] = moved[cell - lo : cell - lo + 1]
                            adj_c[d, c, pl.ds(r + q, 1), 0:w] = adj[r + q, cell : cell + 1, s : s + w]
                    buf.moved[c, lo:hi, 0:w] = moved
                    sums[q] = add_up(chunk, moved, *sums[q])
            return source(slots[0:2], (r, r + 1), lo, sums)

        stagger(advance, chosen)

    def edge(pieces):
        def advance(p):
            lo, hi = TILE * p, TILE * p + TILE
            sums = [none, none]
            lon = [lon_cells(f, lo) for f in (0, rows - 1, rows)]
            lat = [(opy[r, lo:hi], ody[r, lo:hi]) for r in (0, rows - 1)]
            for chunk in chunks:
                c, s, w = chunk
                for q, r in enumerate((0, rows - 1)):
                    own = sp[r, lo:hi, s : s + w]
                    if q == 0:
                        flux_west = upwind(lon_speed(0, chunk, lo, lon[0]), unpack(plan_pos, chunk, recv_s.at[p, 0]), own)
                        flux = fxs[1, c, lo:hi, 0:w]
                    else:
                        before = lon_speed(rows - 1, chunk, lo, lon[1])
                        flux_west = upwind(before, sp[rows - 2, lo:hi, s : s + w], own)
                        flux = upwind(lon_speed(rows, chunk, lo, lon[2]), own, unpack(plan_neg, chunk, recv_s.at[p, 1]))
                    moved = own - (flux - flux_west) - lat_part(slots[2 + q], r, chunk, lo, own, lat[q], p - 1 not in pieces, p + 1 not in pieces, True)
                    slots[2 + q].moved[c, lo:hi, 0:w] = moved
                    sums[q] = add_up(chunk, moved, *sums[q])
            return source(slots[2:4], (0, rows - 1), lo, sums)

        for p in pieces:
            settle(recv_s.at[p], recv_sem.at[2 + p])
        stagger(advance, pieces)
        for p in pieces:
            lo, hi = TILE * p, TILE * p + TILE
            for d, (row, plan) in enumerate(((rows - 1, plan_neg), (0, plan_pos))):
                pack(plan, chunks, lambda c, row=row: tt[row, c, 8 + lo : 8 + hi, 0 : chunks[c][2]], send_t.at[p, d])
            for copy in lon_t[p]:
                copy.start()

    def ends_of(groups_of):
        jobs = [(g, d) for g in groups_of for d in range(2)]

        def advance(job):
            g, d = job
            at, sums = slice(TILE * g, TILE * g + TILE), none
            for chunk in chunks:
                c, _, w = chunk
                courant = cst[d, 0, at, 0:w] * tab[1, c, :, 0:w] + cst[d, 1, at, 0:w]
                face_c[d, c, at, 0:w] = courant
                own, halo = own_c[d, c, at, 0:w], halo_c[d, c, at, 0:w]
                flux = upwind(courant, halo, own) if d == 0 else -upwind(courant, own, halo)
                moved = part_c[d, c, at, 0:w] + flux
                part_c[d, c, at, 0:w] = moved
                sums = add_up(chunk, moved, *sums)
            return finish(g, d, sums)

        def finish(g, d, sums):
            at = slice(TILE * g, TILE * g + TILE)
            energy, sums = mean(sums), none
            for chunk in chunks:
                c, _, w = chunk
                mine_c[d, c, at, 0:w], sums = weigh(
                    chunk, part_c[d, c, at, 0:w], adj_c[d, c, at, 0:w], energy, cst[d, 2, at], cst[d, 3, at], cst[d, 4, at], sums
                )
            yield
            coupling = mean(sums)
            for c, _, w in chunks:
                mine_c[d, c, at, 0:w] = mine_c[d, c, at, 0:w] - coupling[:, 0:w]
            yield

        stagger(advance, jobs)
        for g in groups_of:
            for r in range(TILE * g, TILE * g + TILE):
                for c, _, w in chunks:
                    for d, cell in enumerate((0, cells - 1)):
                        if 0 < r < rows - 1:
                            tt[r, c, 8 + cell : 9 + cell, 0:w] = mine_c[d, c, r : r + 1, 0:w]

    def send_ends(g):
        for r in (0, rows - 1):
            if r // TILE == g:
                for c, _, w in chunks:
                    for d, cell in enumerate((0, cells - 1)):
                        mine_c[d, c, r : r + 1, 0:w] = tt[r, c, 8 + cell : 9 + cell, 0:w]
        lat_start(lambda side: [side.second[g]])

    def wait_group(n):
        settle(both.at[:, pl.ds(bounds[n], bounds[n + 1] - bounds[n])], load_sem.at[6 + n])

    wait_group(0)
    for lo in range(0, cells, TILE):
        lon = lon_cells(1, lo)
        for chunk in chunks:
            c, s, w = chunk
            flux = upwind(lon_speed(1, chunk, lo, lon), sp[0, lo : lo + TILE, s : s + w], sp[1, lo : lo + TILE, s : s + w])
            for m in range(2):
                fxs[m, c, lo : lo + TILE, 0:w] = flux

    pl.semaphore_wait(barrier, 2 + has_north.astype(jnp.int32) + has_south.astype(jnp.int32))
    for copy in ahead:
        copy.start()
    lat_start(lambda side: side.small)
    for p in order:
        for copy in lon_s[p]:
            copy.start()
    lat_start(lambda side: side.first)

    firsts = [next(k for k in range(pairs + 1) if 3 + 2 * k >= b) for b in bounds[1:-1]]

    def halo_faces():
        for m, ref in enumerate((face_f, face_i)):
            settle(ref, recv_sem.at[m])
        lat_arrive(lambda side: [copy.wait_recv() for copy in side.small])
        ext[0, 0:1, 0:cells] = face_f[0, TILE - 1 : TILE]
        ext[0, rows + 1 : rows + 2, 0:cells] = face_f[1, 0:1]
        ext[1, 0:1, 0:cells] = sea_of(face_i[0, TILE - 1 : TILE])
        ext[1, rows + 1 : rows + 2, 0:cells] = sea_of(face_i[1, 0:1])
        ext[4, 0:rows, 0:cells] = near_f[0]
        ext[5, 0:rows, 0:cells] = sea_of(near_i[0])
        ext[6, 0:rows, 0:cells] = near_f[1]
        ext[7, 0:rows, 0:cells] = sea_of(near_i[1])
        for n, f in enumerate((0, rows)):
            opened = ext[1, f : f + 1] * ext[1, f + 1 : f + 2]
            ext[10, n : n + 1] = opened
            ext[10, n + 2 : n + 3] = opened * (0.5 * (ext[0, f : f + 1] + ext[0, f + 1 : f + 2]))

        def put_lon(i, block):
            (opx, odx)[i // 2][(0, rows)[i % 2], 0:cells] = block

        spread(turned(ext[10, 0:rows])[0:cells], 4, put_lon)

        def with_ends(own, south, north):
            mine = jnp.where(lane == cells, pltpu.roll(own, cells, axis=1), own)
            other = jnp.where(lane == cells - 1, pltpu.roll(north, cells - 1, axis=1), ahead_of(own))
            return mine, jnp.where(lane == cells, pltpu.roll(south, 1, axis=1), other)

        sea_a, sea_b = with_ends(ext[3, 0:rows], ext[5, 0:rows], ext[7, 0:rows])
        cy_a, cy_b = with_ends(ext[2, 0:rows], ext[4, 0:rows], ext[6, 0:rows])
        closed = jnp.logical_or(
            jnp.logical_and(lane == cells, jnp.logical_not(has_south)),
            jnp.logical_and(lane == cells - 1, jnp.logical_not(has_north)),
        )
        opened = jnp.where(closed, 0.0, sea_a * sea_b)
        drift = jnp.where(closed, 0.0, opened * (0.5 * (cy_a + cy_b)))
        for m, (field, home) in enumerate(((opened, opy), (drift, ody))):
            for d, face in enumerate((cells, cells - 1)):
                cst[d, m] = jnp.broadcast_to(field[:, face : face + 1], (rows, LANES))
            for r in (0, rows - 1):
                home[r, cells - 1 : cells] = cst[1, m, r : r + 1]
        settle(adj.at[pl.ds(0, 2)], load_sem.at[6 + len(groups)])
        for r in (0, rows - 1):
            for c, s, w in chunks:
                for d in range(2):
                    part_c[d, c, r : r + 1, 0:w] = nil[:, 0:w]
                    adj_c[d, c, r : r + 1, 0:w] = nil[:, 0:w]

    cut = pairs // 2 + 1
    every, outer, inner = list(range(tiles)), [0, tiles - 1], list(range(1, tiles - 1))

    def step(chosen):
        def one(k, carry):
            for n, first in enumerate(firsts):
                if chosen != inner:
                    @pl.when(k == first)
                    def _(n=n):
                        wait_group(n + 1)

            row_pair(1 + 2 * k, chosen)
            return carry

        return one

    lax.fori_loop(0, cut, step(every), 0)
    lax.fori_loop(cut, pairs, step(outer), 0)
    for n in range(len(firsts)):
        if firsts[n] >= pairs:
            wait_group(n + 1)
    halo_faces()
    edge(inner)
    for g in range(tops):
        first_arrives(g)
    ends_of(range(tops))
    for g in range(1, tops - 1):
        send_ends(g)
    edge(outer)
    for g in (0, tops - 1):
        send_ends(g)
    lax.fori_loop(cut, pairs, step(inner), 0)

    def back(r, count, chunk, lo, west_t, east_t):
        c, s, w = chunk
        at = lambda first: pl.ds(lo + first, TILE)
        here, step = west_t, tt[r, c, at(8), 0:w] - west_t
        speed = cxs[r, c, at(0), 0:w]
        for q in range(r, r + count):
            here = tt[q, c, at(8), 0:w]
            value = here + jnp.minimum(speed, 0.0) * step
            step = (east_t if q == r + count - 1 else tt[q + 1, c, at(8), 0:w]) - here
            speed = cxs[q + 1, c, at(0), 0:w]
            value = value + jnp.maximum(speed, 0.0) * step
            value = value + jnp.maximum(cys[q, c, at(8), 0:w], 0.0) * (tt[q, c, at(9), 0:w] - here)
            value = value + jnp.minimum(cys[q, c, at(7), 0:w], 0.0) * (here - tt[q, c, at(7), 0:w])
            done[q, at(0), s : s + w] = value

    def back_tile(a, carry):
        lo = pl.multiple_of(a * TILE, TILE)
        for chunk in chunks:
            c, _, w = chunk
            back(1, rows - 2, chunk, lo, tt[0, c, pl.ds(lo + 8, TILE), 0:w], tt[rows - 1, c, pl.ds(lo + 8, TILE), 0:w])
        return carry

    lax.fori_loop(0, tiles, back_tile, 0)
    for g in range(tops):
        second_arrives(g)
        rows_of = slice(TILE * g, TILE * g + TILE)
        for d in range(2):
            for c, _, w in chunks:
                courant = face_c[d, c, rows_of, 0:w]
                step = next_c[d, c, rows_of, 0:w] - mine_c[d, c, rows_of, 0:w]
                if d == 0:
                    part_c[d, c, rows_of, 0:w] = -jnp.minimum(courant, 0.0) * step
                else:
                    part_c[d, c, rows_of, 0:w] = jnp.maximum(courant, 0.0) * step
        for r in range(TILE * g, TILE * g + TILE):
            for c, s, w in chunks:
                for d, cell in enumerate((0, cells - 1)):
                    if 0 < r < rows - 1:
                        done[r, cell : cell + 1, s : s + w] = done[r, cell : cell + 1, s : s + w] + part_c[d, c, r : r + 1, 0:w]
                    else:
                        beyond = (7, 8 + cells)[d]
                        tt[r, c, beyond : beyond + 1, 0:w] = next_c[d, c, r : r + 1, 0:w]
    for p in order:
        settle(recv_t.at[p], recv_sem.at[2 + tiles + p])
        lo, hi = TILE * p, TILE * p + TILE
        for chunk in chunks:
            c, _, w = chunk
            back(0, 1, chunk, lo, unpack(plan_neg, chunk, recv_t.at[p, 0]), tt[1, c, 8 + lo : 8 + hi, 0:w])
            back(rows - 1, 1, chunk, lo, tt[rows - 2, c, 8 + lo : 8 + hi, 0:w], unpack(plan_pos, chunk, recv_t.at[p, 1]))

    for n, ref in enumerate((face_f, face_i, send_s, send_t)):
        settle(ref, send_sem.at[n])
    for d, side in enumerate(lat_all):
        @pl.when(side.there)
        def _(d=d, side=side):
            for copy in side.small:
                copy.wait_send()
            settle(own_c.at[1 - d], send_sem.at[side.out + 2])
            settle(mine_c.at[1 - d], send_sem.at[side.out + 3])


def keep(array):
    return pltpu.with_memory_space_constraint(array, pltpu.HBM)


def round_up(value, step):
    return (value + step - 1) // step * step


def body(nx, ny, spectrum, adjoint_in, cx, cy, wx, wy, land, ice, speed, growth, diss):
    rows, cells, bins = spectrum.shape
    freqs = speed.shape[0]
    angles = 2.0 * math.pi / DIRS * (np.arange(DIRS) + 0.5)
    cosine, sine = (np.repeat(f(angles), freqs) for f in (np.cos, np.sin))
    plan_pos, plan_neg = slot_plan(cosine > -CERTAIN), slot_plan(cosine < CERTAIN)
    slots = max(len(plan_pos), len(plan_neg))
    many = round_up(freqs, 16)
    hot = (np.arange(many)[:, None] == np.arange(bins)[None] % freqs).astype(np.float32)
    consts = np.concatenate([hot, np.tile(cosine, (TILE, 1)), np.tile(sine, (TILE, 1))]).astype(np.float32)
    tiles, width = cells // TILE, -(-bins // LANES)
    tall = round_up(rows + 2, 8)
    compact = pltpu.VMEM((2, width, rows, LANES), jnp.float32)
    f32 = jnp.float32
    dma = pltpu.SemaphoreType.DMA
    vmem = lambda *shape: pltpu.VMEM(shape, f32)
    return pl.pallas_call(
        functools.partial(kernel, nx, ny, plan_pos, plan_neg),
        out_shape=jax.ShapeDtypeStruct((rows, cells, bins), f32),
        in_specs=[HBM] * 12,
        out_specs=VMEM,
        scratch_shapes=[
            vmem(2, rows, cells, bins),
            vmem(2, rows, 1, bins),
            compact, compact, compact, compact, compact, compact, compact,
            vmem(2, 5, rows, LANES),
            vmem(rows, width, cells + 16, LANES),
            vmem(rows + 1, width, cells, LANES),
            vmem(2, width, cells, LANES),
            vmem(rows, width, cells + 8, LANES),
            vmem(5, width, TILE, LANES),
            vmem(rows + 1, cells, LANES),
            vmem(rows + 1, cells, LANES),
            vmem(rows, cells, LANES),
            vmem(rows, cells, LANES),
            vmem(rows, cells, LANES),
            vmem(rows, cells, LANES),
            vmem(rows, cells, LANES),
            vmem(tiles, 2, slots, TILE, LANES),
            vmem(tiles, 2, slots, TILE, LANES),
            vmem(tiles, 2, slots, TILE, LANES),
            vmem(tiles, 2, slots, TILE, LANES),
            vmem(4, rows, cells),
            pltpu.VMEM((2, rows, cells), jnp.int32),
            vmem(2, rows, cells),
            pltpu.VMEM((2, rows, cells), jnp.int32),
            vmem(2, TILE, cells),
            pltpu.VMEM((2, TILE, cells), jnp.int32),
            vmem(3, 1, freqs),
            vmem(many + 2 * TILE, bins),
            vmem(3 * TILE, many),
            vmem(11, tall, LANES),
            vmem(16, width, cells + 8, LANES),
            dma((11,)),
            dma((12,)),
            dma((2 + 2 * tiles + 4 + 4 * (rows // TILE),)),
        ],
        compiler_params=pltpu.CompilerParams(
            collective_id=0, has_side_effects=True, vmem_limit_bytes=40 * 2**20
        ),
        name="step",
    )(*map(keep, (spectrum, adjoint_in, cx, cy, wx, wy, land, ice)),
      *map(keep, (speed.reshape(1, -1), growth.reshape(1, -1), diss.reshape(1, -1), jnp.asarray(consts))))


def solution(mesh):
    grid = P("gx", "gy")
    field = P("gx", "gy", None)
    return jax.shard_map(
        functools.partial(body, mesh.shape["gx"], mesh.shape["gy"]),
        mesh=mesh,
        in_specs=(field, field) + (grid,) * 6 + (P(), P(), P()),
        out_specs=field,
        check_vma=False,
    )
```

```python
import functools
import math
from types import SimpleNamespace

import jax
import jax.numpy as jnp
import numpy as np
from jax import lax
from jax.experimental import pallas as pl
from jax.experimental.pallas import tpu as pltpu
from jax.sharding import PartitionSpec as P

DIRS = 36
LANES = 128
TILE = 8
CERTAIN = 0.81
HBM = pl.BlockSpec(memory_space=pltpu.HBM)
VMEM = pl.BlockSpec(memory_space=pltpu.VMEM)
MESH = pl.DeviceIdType.MESH


def lane_chunks(bins):
    return [(c, s, min(LANES, bins - s)) for c, s in enumerate(range(0, bins, LANES))]


def slot_plan(need):
    parts = []
    for c, s, w in lane_chunks(len(need)):
        lane = 0
        while lane < w:
            if not need[s + lane]:
                lane += 1
                continue
            first = lane
            while lane < w and need[s + lane]:
                lane += 1
            parts.append((c, first, lane, w))
    parts.sort(key=lambda p: (p[3] == LANES, p[1] - p[2]))
    slots, used = [], []
    for c, first, last, w in parts:
        size = last - first
        for n, busy in enumerate(used):
            if not busy[first:last].any():
                shift = 0
            elif w == LANES:
                starts = [k for k in range(LANES - size + 1) if not busy[k : k + size].any()]
                if not starts:
                    continue
                shift = starts[0] - first
            else:
                continue
            busy[first + shift : last + shift] = True
            slots[n].append((c, first, last, shift % LANES))
            break
        else:
            busy = np.zeros(LANES, bool)
            busy[first:last] = True
            used.append(busy)
            slots.append([(c, first, last, 0)])
    return slots


def repeat(value, count):
    return value if count == 1 else jnp.concatenate([value] * count, axis=0)


def between(first, last):
    lane = lax.broadcasted_iota(jnp.int32, (TILE, LANES), 1)
    return jnp.logical_and(lane >= first, lane < last)


def pack(plan, chunks, load, out):
    for n, parts in enumerate(plan):
        value, late = None, None
        for c, first, last, shift in parts:
            w = chunks[c][2]
            if w < LANES:
                late = (c, w)
                continue
            part = load(c)
            if shift:
                part = pltpu.roll(part, shift, axis=1)
            begin = (first + shift) % LANES
            value = part if value is None else jnp.where(between(begin, begin + last - first), part, value)
        if value is not None:
            out[n] = value
        if late is not None:
            out[n, :, 0 : late[1]] = load(late[0])


def unpack(plan, chunk, slots):
    c, _, w = chunk
    value = jnp.zeros((TILE, w), jnp.float32)
    for n, parts in enumerate(plan):
        for chunk_of, first, last, shift in parts:
            if chunk_of != c:
                continue
            if w < LANES:
                part = slots[n, :, 0:w]
                if last - first < w:
                    part = jnp.where(between(first, last)[:, 0:w], part, 0.0)
                value = part
                continue
            part = slots[n]
            if shift:
                part = pltpu.roll(part, LANES - shift, axis=1)
            value = part if last - first == LANES else jnp.where(between(first, last), part, value)
    return value


def split3(value):
    high = value.astype(jnp.bfloat16).astype(jnp.float32)
    rest = value - high
    mid = rest.astype(jnp.bfloat16).astype(jnp.float32)
    return [high, mid, rest - mid]


def kernel(
    nx, ny, plan_pos, plan_neg,
    spectrum, adjoint, cx_h, cy_h, wx_h, wy_h, land_h, ice_h, speed_h, growth_h, diss_h, consts_h,
    done,
    both, rim, own_c, halo_c, adj_c, part_c, face_c, mine_c, next_c, cst, tt, cxs, fxs, cys, tab, opx, odx, opy, ody, wxs, wys, seas,
    send_s, recv_s, send_t, recv_t, mine_f, mine_i, near_f, near_i, face_f, face_i, coeffs, consts, params, ext, bufs, load_sem, send_sem, recv_sem,
):
    gx, gy = lax.axis_index("gx"), lax.axis_index("gy")
    rows, cells, bins = adjoint.shape
    east, west = lax.rem(gx + 1, nx), lax.rem(gx + nx - 1, nx)
    has_north, has_south = gy < ny - 1, gy > 0
    chunks = lane_chunks(bins)
    tiles = cells // TILE
    f32 = jnp.float32
    sp, adj = both.at[0], both.at[1]

    cx, cy, wx, wy = (mine_f.at[m] for m in range(4))
    land, ice = (mine_i.at[m] for m in range(2))
    speed, growth, diss = (coeffs.at[m] for m in range(3))
    pairs = (rows - 2) // 2
    bounds = [1, 4, 10, 16, rows - 1]
    local = lambda src, dst, n: pltpu.make_async_copy(src, dst, load_sem.at[n])
    ends = [local(spectrum.at[r], sp.at[r], 0) for r in (0, rows - 1)]
    small = [
        local(src, dst, n)
        for src, dst, n in (
            (cx_h, cx, 1), (cy_h, cy, 1), (wx_h, wx, 1), (wy_h, wy, 1), (land_h, land, 2), (ice_h, ice, 2),
            (speed_h, speed, 3), (growth_h, growth, 3), (diss_h, diss, 3), (consts_h, consts, 4),
        )
    ]
    rims = [
        local(spectrum.at[:, pl.ds(0, 1), :], rim.at[0], 5),
        local(spectrum.at[:, pl.ds(cells - 1, 1), :], rim.at[1], 5),
    ]
    groups = []
    for n, (a, b) in enumerate(zip(bounds[:-1], bounds[1:])):
        groups.append(
            [local(src.at[pl.ds(a, b - a)], dst.at[pl.ds(a, b - a)], 6 + n) for src, dst in ((spectrum, sp), (adjoint, adj))]
        )
    last_adj = [local(adjoint.at[r], adj.at[r], 6 + len(groups)) for r in (0, rows - 1)]
    for copy in ends + small + rims:
        copy.start()

    barrier = pltpu.get_barrier_semaphore()
    for where in (east, west):
        pl.semaphore_signal(barrier, inc=1, device_id={"gx": where}, device_id_type=MESH)

    @pl.when(has_north)
    def _():
        pl.semaphore_signal(barrier, inc=1, device_id={"gy": gy + 1}, device_id_type=MESH)

    @pl.when(has_south)
    def _():
        pl.semaphore_signal(barrier, inc=1, device_id={"gy": gy - 1}, device_id_type=MESH)

    for group in groups:
        for copy in group:
            copy.start()
    for copy in last_adj:
        copy.start()

    def far(src, dst, out, n, axis, where):
        return pltpu.make_async_remote_copy(
            src_ref=src, dst_ref=dst, send_sem=send_sem.at[out], recv_sem=recv_sem.at[n],
            device_id={axis: where}, device_id_type=MESH,
        )

    def settle(ref, sem):
        pltpu.make_async_copy(ref, ref, sem).wait()

    order = list(range(1, tiles - 1)) + [0, tiles - 1]
    ahead = []
    for m, (src, dst) in enumerate(((cx, face_f), (land, face_i))):
        ahead.append(far(src.at[pl.ds(rows - TILE, TILE)], dst.at[0], m, m, "gx", east))
        ahead.append(far(src.at[pl.ds(0, TILE)], dst.at[1], m, m, "gx", west))
    lon_s, lon_t = (
        [[far(src.at[p, d], dst.at[p, d], 2 + m, 2 + m * tiles + p, "gx", (east, west)[d]) for d in range(2)] for p in range(tiles)]
        for m, (src, dst) in enumerate(((send_s, recv_s), (send_t, recv_t)))
    )
    tops = rows // TILE
    span = lambda g: pl.ds(TILE * g, TILE)
    lat_all = []
    for d, (where, there, back_there) in enumerate(((gy + 1, has_north, has_south), (gy - 1, has_south, has_north))):
        sem = 2 + 2 * tiles + (2 + 2 * tops) * d
        away = lambda src, dst, out, n, where=where, d=d, sem=sem: far(src, dst, 4 + 4 * d + out, sem + n, "gy", where)
        lat_all.append(SimpleNamespace(
            there=there, back_there=back_there, out=4 + 4 * d,
            small=[away(cy, near_f.at[d], 0, 0), away(land, near_i.at[d], 1, 1)],
            first=[away(own_c.at[1 - d, :, span(g)], halo_c.at[d, :, span(g)], 2, 2 + g) for g in range(tops)],
            second=[away(mine_c.at[1 - d, :, span(g)], next_c.at[d, :, span(g)], 3, 2 + tops + g) for g in range(tops)],
        ))

    def lat_start(pick):
        for side in lat_all:
            @pl.when(side.there)
            def _(side=side):
                for copy in pick(side):
                    copy.start()

    def lat_arrive(pick):
        for side in lat_all:
            @pl.when(side.back_there)
            def _(side=side):
                pick(side)

    def first_arrives(n):
        lat_arrive(lambda side: side.first[n].wait_recv())

    def second_arrives(n):
        lat_arrive(lambda side: side.second[n].wait_recv())

    settle(sp.at[pl.ds(0, 2)], load_sem.at[0])
    for p in range(tiles):
        for d, (row, plan) in enumerate(((rows - 1, plan_pos), (0, plan_neg))):
            load = lambda c, row=row, p=p: sp[row, TILE * p : TILE * p + TILE, chunks[c][1] : chunks[c][1] + chunks[c][2]]
            pack(plan, chunks, load, send_s.at[p, d])
    for n, ref in enumerate((mine_f, mine_i, coeffs, consts, rim)):
        settle(ref, load_sem.at[1 + n])

    nil = jnp.zeros((1, LANES), f32)

    def prepare(r, carry):
        for c, s, w in chunks:
            for d in range(2):
                own_c[d, c, pl.ds(r, 1), 0:w] = rim[d, r, :, s : s + w]
            tt[r, c, 7:8] = nil
            tt[r, c, 8 + cells : 9 + cells] = nil
            cys[r, c, 7:8] = nil
        return carry

    lax.fori_loop(0, rows, prepare, 0)
    for q in range(2):
        for c, _, _ in chunks:
            bufs[4 * q, c, cells : cells + 1] = nil
            bufs[4 * q + 1, c, 7:8] = nil
    freqs = coeffs.shape[2]
    params[...] = jnp.zeros(params.shape, f32)
    for m, ref in enumerate((speed, growth, diss)):
        params[TILE * m : TILE * m + TILE, 0:freqs] = jnp.broadcast_to(ref[...], (TILE, freqs))
    many = params.shape[1]
    hot = consts[0:many].astype(jnp.bfloat16)
    by_bin = sum(
        jnp.dot(part.astype(jnp.bfloat16), hot, preferred_element_type=f32) for part in split3(params[...])
    )
    cosine, sine = consts[many : many + TILE], consts[many + TILE : many + 2 * TILE]
    for c, s, w in chunks:
        cs = slice(s, s + w)
        tab[0, c, :, 0:w] = by_bin[0:TILE, cs] * cosine[:, cs]
        tab[1, c, :, 0:w] = by_bin[0:TILE, cs] * sine[:, cs]
        tab[2, c, :, 0:w] = by_bin[TILE : 2 * TILE, cs] * cosine[:, cs]
        tab[3, c, :, 0:w] = by_bin[TILE : 2 * TILE, cs] * sine[:, cs]
        tab[4, c, :, 0:w] = by_bin[2 * TILE : 3 * TILE, cs]

    sub = lax.broadcasted_iota(jnp.int32, (LANES, 2 * LANES), 0)
    half = (lax.broadcasted_iota(jnp.int32, (LANES, 2 * LANES), 1) >= LANES).astype(jnp.int32)
    row_of = jnp.where(sub < rows, sub, jnp.where(sub < 2 * rows, sub - rows, jnp.where(sub < 3 * rows, sub - 2 * rows, -2)))
    row_of = row_of - half

    def turned(field):
        stack = split3(field)
        stack.append(jnp.zeros((LANES - 3 * rows, LANES), f32))
        return jnp.concatenate(stack, axis=0).T

    def spread(lhs, count, put):
        lhs = lhs.astype(jnp.bfloat16)
        for n in range(count // 2):
            pick = jnp.where(row_of == 2 * n, 1.0, 0.0).astype(jnp.bfloat16)
            out = jnp.dot(lhs, pick, preferred_element_type=f32)
            put(2 * n, out[:, 0:LANES])
            put(2 * n + 1, out[:, LANES:])

    sea_of = lambda mask: (1 - mask).astype(f32)
    ext[...] = jnp.zeros(ext.shape, f32)
    ice_free = sea_of(ice[...])
    ext[0, 1 : rows + 1, 0:cells] = cx[...]
    ext[1, 1 : rows + 1, 0:cells] = sea_of(land[...])
    ext[2, 0:rows, 0:cells] = cy[...]
    ext[3, 0:rows, 0:cells] = sea_of(land[...])
    windy = ice_free * sea_of(land[...])
    ext[8, 0:rows, 0:cells] = wx[...] * windy
    ext[9, 0:rows, 0:cells] = wy[...] * windy
    lane = lax.broadcasted_iota(jnp.int32, (rows, LANES), 1)
    sea, drift = ext[3, 0:rows], ext[2, 0:rows]
    opened_x = ext[1, 0:rows] * ext[1, 1 : rows + 1]
    ahead_of = lambda value: pltpu.roll(value, LANES - 1, axis=1)
    opened_y = sea * ahead_of(sea)
    fields = [
        opened_x, opened_x * (0.5 * (ext[0, 0:rows] + ext[0, 1 : rows + 1])),
        opened_y, opened_y * (0.5 * (drift + ahead_of(drift))),
        ext[8, 0:rows], ext[9, 0:rows], sea,
    ]
    homes = (opx, odx, opy, ody, wxs, wys, seas)

    def put_all(i, block):
        for k, home in enumerate(homes):
            home[i, 0:cells] = block[k * cells : (k + 1) * cells]

    spread(jnp.concatenate([turned(f)[0:cells] for f in fields], axis=0), rows, put_all)

    for m, field in enumerate((ext[8, 0:rows], ext[9, 0:rows], sea)):
        for d, cell in enumerate((0, cells - 1)):
            cst[d, 2 + m] = jnp.broadcast_to(field[:, cell : cell + 1], (rows, LANES))
    for d, there in enumerate((has_south, has_north)):
        @pl.when(jnp.logical_not(there))
        def _(d=d):
            halo_c[d] = jnp.zeros(halo_c.shape[1:], f32)
            next_c[d] = jnp.zeros(next_c.shape[1:], f32)

    def lat_part(buf, r, chunk, lo, own, fields, first, last, ends):
        c, s, w = chunk
        hi = lo + TILE
        sine_row = tab[1, c, :, 0:w]
        if first:
            buf.near[c, lo:hi, 0:w] = own
        if not last:
            buf.near[c, hi : hi + TILE, 0:w] = sp[r, hi : hi + TILE, s : s + w]
        elif hi < cells:
            buf.near[c, hi : hi + 1, 0:w] = sp[r, hi : hi + 1, s : s + w]
        elif ends:
            buf.near[c, hi : hi + 1, 0:w] = halo_c[1, c, r : r + 1, 0:w]
        upper = buf.near[c, lo + 1 : hi + 1, 0:w]
        courant = fields[0][:, 0:w] * sine_row + fields[1][:, 0:w]
        cys[r, c, 8 + lo : 8 + hi, 0:w] = courant
        fy = courant * jnp.where(courant > 0, own, upper)
        buf.flux[c, 8 + lo : 8 + hi, 0:w] = fy
        if first and (lo or ends):
            if lo:
                low = opy[r, lo - 1 : lo, 0:w] * sine_row[0:1] + ody[r, lo - 1 : lo, 0:w]
                below = sp[r, lo - 1 : lo, s : s + w]
            else:
                low = cst[0, 0, r : r + 1, 0:w] * sine_row[0:1] + cst[0, 1, r : r + 1, 0:w]
                below = halo_c[0, c, r : r + 1, 0:w]
                cys[r, c, 7 + lo : 8 + lo, 0:w] = low
            buf.flux[c, 7 + lo : 8 + lo, 0:w] = low * jnp.where(low > 0, below, own[0:1])
        return fy - buf.flux[c, 7 + lo : 7 + hi, 0:w]

    def lon_cells(f, lo):
        return opx[f, lo : lo + TILE], odx[f, lo : lo + TILE]

    def lon_speed(f, chunk, lo, fields):
        c, _, w = chunk
        speed = fields[0][:, 0:w] * tab[0, c, :, 0:w] + fields[1][:, 0:w]
        cxs[f, c, lo : lo + TILE, 0:w] = speed
        return speed

    def upwind(speed, here, there):
        return speed * jnp.where(speed > 0, here, there)

    def gather(totals, rest):
        value = jnp.sum(totals, axis=1, keepdims=True)
        return value if rest is None else value + rest

    def mean(sums):
        return jnp.broadcast_to(gather(*sums) * (1.0 / bins), (TILE, LANES))

    def weigh(chunk, advected, incoming, energy, wind_x, wind_y, open_sea, sums):
        c, _, w = chunk
        blow = wind_x[:, 0:w] * tab[2, c, :, 0:w] + wind_y[:, 0:w] * tab[3, c, :, 0:w]
        gain = open_sea[:, 0:w] + jnp.maximum(blow, 0.0)
        scaled = tab[4, c, :, 0:w] * advected
        damp = 1.0 + energy[:, 0:w] * scaled
        weighted = incoming * gain / (damp * damp)
        return weighted, add_up(chunk, weighted * scaled * advected, *sums)

    def add_up(chunk, value, total, rest):
        if chunk[2] == LANES:
            return total + value, rest
        return total, jnp.sum(value, axis=1, keepdims=True)

    none = (jnp.zeros((TILE, LANES), f32), None)
    slots = [SimpleNamespace(near=bufs.at[4 * q], flux=bufs.at[4 * q + 1], moved=bufs.at[4 * q + 2], weight=bufs.at[4 * q + 3]) for q in range(4)]

    def source(bufs_of, rows_of, lo, sums):
        hi = lo + TILE
        energy = [mean(each) for each in sums]
        sums = [none for _ in sums]
        fields = [(wxs[r, lo:hi], wys[r, lo:hi], seas[r, lo:hi]) for r in rows_of]
        for chunk in chunks:
            c, s, w = chunk
            for q, (buf, r) in enumerate(zip(bufs_of, rows_of)):
                weighted, sums[q] = weigh(chunk, buf.moved[c, lo:hi, 0:w], adj[r, lo:hi, s : s + w], energy[q], *fields[q], sums[q])
                buf.weight[c, lo:hi, 0:w] = weighted
        yield
        coupling = [mean(each) for each in sums]
        for c, s, w in chunks:
            for q, (buf, r) in enumerate(zip(bufs_of, rows_of)):
                tt[r, c, 8 + lo : 8 + hi, 0:w] = buf.weight[c, lo:hi, 0:w] - coupling[q][:, 0:w]
        yield

    def stagger(first, jobs):
        running = []
        for step in range(len(jobs) + 2):
            if step < len(jobs):
                running.append(first(jobs[step]))
            for n in (step - 1, step - 2):
                if 0 <= n < len(jobs):
                    next(running[n])

    def row_pair(r, chosen):
        def advance(a):
            lo, hi = TILE * a, TILE * a + TILE
            first, last = a - 1 not in chosen, a + 1 not in chosen
            sums = [none, none]
            lon = [lon_cells(r + q + 1, lo) for q in range(2)]
            lat = [(opy[r + q, lo:hi], ody[r + q, lo:hi]) for q in range(2)]
            for chunk in chunks:
                c, s, w = chunk
                own = [sp[r + q, lo:hi, s : s + w] for q in range(3)]
                flux_west = fxs[0, c, lo:hi, 0:w]
                for q in range(2):
                    buf = slots[q]
                    flux = upwind(lon_speed(r + q + 1, chunk, lo, lon[q]), own[q], own[q + 1])
                    if q:
                        fxs[0, c, lo:hi, 0:w] = flux
                    moved = own[q] - (flux - flux_west) - lat_part(buf, r + q, chunk, lo, own[q], lat[q], first, last, False)
                    flux_west = flux
                    for d, cell in enumerate((0, cells - 1)):
                        if cell // TILE == a:
                            part_c[d, c, pl.ds(r + q, 1), 0:w] = moved[cell - lo : cell - lo + 1]
                            adj_c[d, c, pl.ds(r + q, 1), 0:w] = adj[r + q, cell : cell + 1, s : s + w]
                    buf.moved[c, lo:hi, 0:w] = moved
                    sums[q] = add_up(chunk, moved, *sums[q])
            return source(slots[0:2], (r, r + 1), lo, sums)

        stagger(advance, chosen)

    def edge(pieces):
        def advance(p):
            lo, hi = TILE * p, TILE * p + TILE
            sums = [none, none]
            lon = [lon_cells(f, lo) for f in (0, rows - 1, rows)]
            lat = [(opy[r, lo:hi], ody[r, lo:hi]) for r in (0, rows - 1)]
            for chunk in chunks:
                c, s, w = chunk
                for q, r in enumerate((0, rows - 1)):
                    own = sp[r, lo:hi, s : s + w]
                    if q == 0:
                        flux_west = upwind(lon_speed(0, chunk, lo, lon[0]), unpack(plan_pos, chunk, recv_s.at[p, 0]), own)
                        flux = fxs[1, c, lo:hi, 0:w]
                    else:
                        before = lon_speed(rows - 1, chunk, lo, lon[1])
                        flux_west = upwind(before, sp[rows - 2, lo:hi, s : s + w], own)
                        flux = upwind(lon_speed(rows, chunk, lo, lon[2]), own, unpack(plan_neg, chunk, recv_s.at[p, 1]))
                    moved = own - (flux - flux_west) - lat_part(slots[2 + q], r, chunk, lo, own, lat[q], p - 1 not in pieces, p + 1 not in pieces, True)
                    slots[2 + q].moved[c, lo:hi, 0:w] = moved
                    sums[q] = add_up(chunk, moved, *sums[q])
            return source(slots[2:4], (0, rows - 1), lo, sums)

        for p in pieces:
            settle(recv_s.at[p], recv_sem.at[2 + p])
        stagger(advance, pieces)
        for p in pieces:
            lo, hi = TILE * p, TILE * p + TILE
            for d, (row, plan) in enumerate(((rows - 1, plan_neg), (0, plan_pos))):
                pack(plan, chunks, lambda c, row=row: tt[row, c, 8 + lo : 8 + hi, 0 : chunks[c][2]], send_t.at[p, d])
            for copy in lon_t[p]:
                copy.start()

    def ends_of(groups_of):
        jobs = [(g, d) for g in groups_of for d in range(2)]

        def advance(job):
            g, d = job
            at, sums = slice(TILE * g, TILE * g + TILE), none
            for chunk in chunks:
                c, _, w = chunk
                courant = cst[d, 0, at, 0:w] * tab[1, c, :, 0:w] + cst[d, 1, at, 0:w]
                face_c[d, c, at, 0:w] = courant
                own, halo = own_c[d, c, at, 0:w], halo_c[d, c, at, 0:w]
                flux = upwind(courant, halo, own) if d == 0 else -upwind(courant, own, halo)
                moved = part_c[d, c, at, 0:w] + flux
                part_c[d, c, at, 0:w] = moved
                sums = add_up(chunk, moved, *sums)
            return finish(g, d, sums)

        def finish(g, d, sums):
            at = slice(TILE * g, TILE * g + TILE)
            energy, sums = mean(sums), none
            for chunk in chunks:
                c, _, w = chunk
                mine_c[d, c, at, 0:w], sums = weigh(
                    chunk, part_c[d, c, at, 0:w], adj_c[d, c, at, 0:w], energy, cst[d, 2, at], cst[d, 3, at], cst[d, 4, at], sums
                )
            yield
            coupling = mean(sums)
            for c, _, w in chunks:
                mine_c[d, c, at, 0:w] = mine_c[d, c, at, 0:w] - coupling[:, 0:w]
            yield

        stagger(advance, jobs)
        for g in groups_of:
            for r in range(TILE * g, TILE * g + TILE):
                for c, _, w in chunks:
                    for d, cell in enumerate((0, cells - 1)):
                        if 0 < r < rows - 1:
                            tt[r, c, 8 + cell : 9 + cell, 0:w] = mine_c[d, c, r : r + 1, 0:w]

    def send_ends(g):
        for r in (0, rows - 1):
            if r // TILE == g:
                for c, _, w in chunks:
                    for d, cell in enumerate((0, cells - 1)):
                        mine_c[d, c, r : r + 1, 0:w] = tt[r, c, 8 + cell : 9 + cell, 0:w]
        lat_start(lambda side: [side.second[g]])

    def wait_group(n):
        settle(both.at[:, pl.ds(bounds[n], bounds[n + 1] - bounds[n])], load_sem.at[6 + n])

    wait_group(0)
    for lo in range(0, cells, TILE):
        lon = lon_cells(1, lo)
        for chunk in chunks:
            c, s, w = chunk
            flux = upwind(lon_speed(1, chunk, lo, lon), sp[0, lo : lo + TILE, s : s + w], sp[1, lo : lo + TILE, s : s + w])
            for m in range(2):
                fxs[m, c, lo : lo + TILE, 0:w] = flux

    pl.semaphore_wait(barrier, 2 + has_north.astype(jnp.int32) + has_south.astype(jnp.int32))
    for copy in ahead:
        copy.start()
    lat_start(lambda side: side.small)
    for p in order:
        for copy in lon_s[p]:
            copy.start()
    lat_start(lambda side: side.first)

    firsts = [next(k for k in range(pairs + 1) if 3 + 2 * k >= b) for b in bounds[1:-1]]

    def halo_faces():
        for m, ref in enumerate((face_f, face_i)):
            settle(ref, recv_sem.at[m])
        lat_arrive(lambda side: [copy.wait_recv() for copy in side.small])
        ext[0, 0:1, 0:cells] = face_f[0, TILE - 1 : TILE]
        ext[0, rows + 1 : rows + 2, 0:cells] = face_f[1, 0:1]
        ext[1, 0:1, 0:cells] = sea_of(face_i[0, TILE - 1 : TILE])
        ext[1, rows + 1 : rows + 2, 0:cells] = sea_of(face_i[1, 0:1])
        ext[4, 0:rows, 0:cells] = near_f[0]
        ext[5, 0:rows, 0:cells] = sea_of(near_i[0])
        ext[6, 0:rows, 0:cells] = near_f[1]
        ext[7, 0:rows, 0:cells] = sea_of(near_i[1])
        for n, f in enumerate((0, rows)):
            opened = ext[1, f : f + 1] * ext[1, f + 1 : f + 2]
            ext[10, n : n + 1] = opened
            ext[10, n + 2 : n + 3] = opened * (0.5 * (ext[0, f : f + 1] + ext[0, f + 1 : f + 2]))

        def put_lon(i, block):
            (opx, odx)[i // 2][(0, rows)[i % 2], 0:cells] = block

        spread(turned(ext[10, 0:rows])[0:cells], 4, put_lon)

        def with_ends(own, south, north):
            mine = jnp.where(lane == cells, pltpu.roll(own, cells, axis=1), own)
            other = jnp.where(lane == cells - 1, pltpu.roll(north, cells - 1, axis=1), ahead_of(own))
            return mine, jnp.where(lane == cells, pltpu.roll(south, 1, axis=1), other)

        sea_a, sea_b = with_ends(ext[3, 0:rows], ext[5, 0:rows], ext[7, 0:rows])
        cy_a, cy_b = with_ends(ext[2, 0:rows], ext[4, 0:rows], ext[6, 0:rows])
        closed = jnp.logical_or(
            jnp.logical_and(lane == cells, jnp.logical_not(has_south)),
            jnp.logical_and(lane == cells - 1, jnp.logical_not(has_north)),
        )
        opened = jnp.where(closed, 0.0, sea_a * sea_b)
        drift = jnp.where(closed, 0.0, opened * (0.5 * (cy_a + cy_b)))
        for m, (field, home) in enumerate(((opened, opy), (drift, ody))):
            for d, face in enumerate((cells, cells - 1)):
                cst[d, m] = jnp.broadcast_to(field[:, face : face + 1], (rows, LANES))
            for r in (0, rows - 1):
                home[r, cells - 1 : cells] = cst[1, m, r : r + 1]
        settle(adj.at[pl.ds(0, 2)], load_sem.at[6 + len(groups)])
        for r in (0, rows - 1):
            for c, s, w in chunks:
                for d in range(2):
                    part_c[d, c, r : r + 1, 0:w] = nil[:, 0:w]
                    adj_c[d, c, r : r + 1, 0:w] = nil[:, 0:w]

    cut = pairs // 2
    every, outer, inner = list(range(tiles)), [0, tiles - 1], list(range(1, tiles - 1))

    def step(chosen):
        def one(k, carry):
            for n, first in enumerate(firsts):
                if chosen != inner:
                    @pl.when(k == first)
                    def _(n=n):
                        wait_group(n + 1)

            row_pair(1 + 2 * k, chosen)
            return carry

        return one

    lax.fori_loop(0, cut, step(every), 0)
    lax.fori_loop(cut, pairs, step(outer), 0)
    for n in range(len(firsts)):
        if firsts[n] >= pairs:
            wait_group(n + 1)
    halo_faces()
    edge(inner)
    for g in range(tops):
        first_arrives(g)
    ends_of(range(tops))
    for g in range(1, tops - 1):
        send_ends(g)
    edge(outer)
    for g in (0, tops - 1):
        send_ends(g)
    lax.fori_loop(cut, pairs, step(inner), 0)

    def back(r, count, chunk, lo, west_t, east_t):
        c, s, w = chunk
        at = lambda first: pl.ds(lo + first, TILE)
        here, step = west_t, tt[r, c, at(8), 0:w] - west_t
        speed = cxs[r, c, at(0), 0:w]
        for q in range(r, r + count):
            here = tt[q, c, at(8), 0:w]
            value = here + jnp.minimum(speed, 0.0) * step
            step = (east_t if q == r + count - 1 else tt[q + 1, c, at(8), 0:w]) - here
            speed = cxs[q + 1, c, at(0), 0:w]
            value = value + jnp.maximum(speed, 0.0) * step
            value = value + jnp.maximum(cys[q, c, at(8), 0:w], 0.0) * (tt[q, c, at(9), 0:w] - here)
            value = value + jnp.minimum(cys[q, c, at(7), 0:w], 0.0) * (here - tt[q, c, at(7), 0:w])
            done[q, at(0), s : s + w] = value

    def back_tile(a, carry):
        lo = pl.multiple_of(a * TILE, TILE)
        for chunk in chunks:
            c, _, w = chunk
            back(1, rows - 2, chunk, lo, tt[0, c, pl.ds(lo + 8, TILE), 0:w], tt[rows - 1, c, pl.ds(lo + 8, TILE), 0:w])
        return carry

    lax.fori_loop(0, tiles, back_tile, 0)
    for g in range(tops):
        second_arrives(g)
        rows_of = slice(TILE * g, TILE * g + TILE)
        for d in range(2):
            for c, _, w in chunks:
                courant = face_c[d, c, rows_of, 0:w]
                step = next_c[d, c, rows_of, 0:w] - mine_c[d, c, rows_of, 0:w]
                if d == 0:
                    part_c[d, c, rows_of, 0:w] = -jnp.minimum(courant, 0.0) * step
                else:
                    part_c[d, c, rows_of, 0:w] = jnp.maximum(courant, 0.0) * step
        for r in range(TILE * g, TILE * g + TILE):
            for c, s, w in chunks:
                for d, cell in enumerate((0, cells - 1)):
                    if 0 < r < rows - 1:
                        done[r, cell : cell + 1, s : s + w] = done[r, cell : cell + 1, s : s + w] + part_c[d, c, r : r + 1, 0:w]
                    else:
                        beyond = (7, 8 + cells)[d]
                        tt[r, c, beyond : beyond + 1, 0:w] = next_c[d, c, r : r + 1, 0:w]
    for p in order:
        settle(recv_t.at[p], recv_sem.at[2 + tiles + p])
        lo, hi = TILE * p, TILE * p + TILE
        for chunk in chunks:
            c, _, w = chunk
            back(0, 1, chunk, lo, unpack(plan_neg, chunk, recv_t.at[p, 0]), tt[1, c, 8 + lo : 8 + hi, 0:w])
            back(rows - 1, 1, chunk, lo, tt[rows - 2, c, 8 + lo : 8 + hi, 0:w], unpack(plan_pos, chunk, recv_t.at[p, 1]))

    for n, ref in enumerate((face_f, face_i, send_s, send_t)):
        settle(ref, send_sem.at[n])
    for d, side in enumerate(lat_all):
        @pl.when(side.there)
        def _(d=d, side=side):
            for copy in side.small:
                copy.wait_send()
            settle(own_c.at[1 - d], send_sem.at[side.out + 2])
            settle(mine_c.at[1 - d], send_sem.at[side.out + 3])


def keep(array):
    return pltpu.with_memory_space_constraint(array, pltpu.HBM)


def round_up(value, step):
    return (value + step - 1) // step * step


def body(nx, ny, spectrum, adjoint_in, cx, cy, wx, wy, land, ice, speed, growth, diss):
    rows, cells, bins = spectrum.shape
    freqs = speed.shape[0]
    angles = 2.0 * math.pi / DIRS * (np.arange(DIRS) + 0.5)
    cosine, sine = (np.repeat(f(angles), freqs) for f in (np.cos, np.sin))
    plan_pos, plan_neg = slot_plan(cosine > -CERTAIN), slot_plan(cosine < CERTAIN)
    slots = max(len(plan_pos), len(plan_neg))
    many = round_up(freqs, 16)
    hot = (np.arange(many)[:, None] == np.arange(bins)[None] % freqs).astype(np.float32)
    consts = np.concatenate([hot, np.tile(cosine, (TILE, 1)), np.tile(sine, (TILE, 1))]).astype(np.float32)
    tiles, width = cells // TILE, -(-bins // LANES)
    tall = round_up(rows + 2, 8)
    compact = pltpu.VMEM((2, width, rows, LANES), jnp.float32)
    f32 = jnp.float32
    dma = pltpu.SemaphoreType.DMA
    vmem = lambda *shape: pltpu.VMEM(shape, f32)
    return pl.pallas_call(
        functools.partial(kernel, nx, ny, plan_pos, plan_neg),
        out_shape=jax.ShapeDtypeStruct((rows, cells, bins), f32),
        in_specs=[HBM] * 12,
        out_specs=VMEM,
        scratch_shapes=[
            vmem(2, rows, cells, bins),
            vmem(2, rows, 1, bins),
            compact, compact, compact, compact, compact, compact, compact,
            vmem(2, 5, rows, LANES),
            vmem(rows, width, cells + 16, LANES),
            vmem(rows + 1, width, cells, LANES),
            vmem(2, width, cells, LANES),
            vmem(rows, width, cells + 8, LANES),
            vmem(5, width, TILE, LANES),
            vmem(rows + 1, cells, LANES),
            vmem(rows + 1, cells, LANES),
            vmem(rows, cells, LANES),
            vmem(rows, cells, LANES),
            vmem(rows, cells, LANES),
            vmem(rows, cells, LANES),
            vmem(rows, cells, LANES),
            vmem(tiles, 2, slots, TILE, LANES),
            vmem(tiles, 2, slots, TILE, LANES),
            vmem(tiles, 2, slots, TILE, LANES),
            vmem(tiles, 2, slots, TILE, LANES),
            vmem(4, rows, cells),
            pltpu.VMEM((2, rows, cells), jnp.int32),
            vmem(2, rows, cells),
            pltpu.VMEM((2, rows, cells), jnp.int32),
            vmem(2, TILE, cells),
            pltpu.VMEM((2, TILE, cells), jnp.int32),
            vmem(3, 1, freqs),
            vmem(many + 2 * TILE, bins),
            vmem(3 * TILE, many),
            vmem(11, tall, LANES),
            vmem(16, width, cells + 8, LANES),
            dma((11,)),
            dma((12,)),
            dma((2 + 2 * tiles + 4 + 4 * (rows // TILE),)),
        ],
        compiler_params=pltpu.CompilerParams(
            collective_id=0, has_side_effects=True, vmem_limit_bytes=40 * 2**20
        ),
        name="step",
    )(*map(keep, (spectrum, adjoint_in, cx, cy, wx, wy, land, ice)),
      *map(keep, (speed.reshape(1, -1), growth.reshape(1, -1), diss.reshape(1, -1), jnp.asarray(consts))))


def solution(mesh):
    grid = P("gx", "gy")
    field = P("gx", "gy", None)
    return jax.shard_map(
        functools.partial(body, mesh.shape["gx"], mesh.shape["gy"]),
        mesh=mesh,
        in_specs=(field, field) + (grid,) * 6 + (P(), P(), P()),
        out_specs=field,
        check_vma=False,
    )
```
